256 devices in a mesh: gx: 64 (over x, z, core), gy: 4 (over y).
Axes of the slice: x: 4, y: 4, z: 8, core: 2. Of those that a mesh axis runs over, the one named last changes fastest.
Arguments:
- measures: bfloat16 [2097152, 128], P(('gx', 'gy')), may hold values from -6 to 6
- row_keys: int32 [2097152], P(('gx', 'gy')), may hold values from 0 to 131071, as said below
- orders: bfloat16 [131072, 128], P(('gx', 'gy')), may hold values from -6 to 6
- heavy_keys: int32 [512], replicated, may hold values from 0 to 131071, as said below
- key_slot: int32 [131072], replicated, may hold values from 0 to 131071, as said below
Outputs:
- result: bfloat16 [131072, 128], P(('gx', 'gy'))
- heavy_report: bfloat16 [512, 128], P(('gx', 'gy'))
- slot_rows: float32 [131072], P(('gx', 'gy'))
The draws below stay inside these ranges and needn't reach their ends.
Inputs may be any that keep to these rules, and one draw needn't show every extreme that they name: `heavy_keys`: for each range block d, entries d * 2 to (d + 1) * 2 - 1 are distinct keys of d * 512 to (d + 1) * 512 - 1. `key_slot`: A permutation. Slot s belongs to owner s // 2048 and to quarter (s // 512) % q with q = 4. Key k lies in range block d = k // 512; every range block has exactly 8 keys with slots of each owner, all in quarter d % q. `row_keys`: in the rows of one device, among rows whose key is not heavy, at most 256 have slots of any one owner and at most 64 distinct keys have slots of any one owner; in every device both bounds are reached by some owner.
All inputs are finite; a program needn't handle non-finite values.
Results may differ from the reference program's by a relative error of at most 0.0021.
Values may be sent and summed in bfloat16 or wider, within the bound.
No kernel may reach another device: no remote copies, remote signals or barrier semaphores. Data moves between devices by JAX's collectives and lax.ppermute only.
A program may use at most 64 MiB of HBM per device.

```python
import jax
import jax.numpy as jnp
from jax import lax

W = 128
ROWS_DEV = 8192
KEY_DEV = 512
HPD = 2
ROWS = 2097152
KEYS = 131072
HEAVY = 512
OWN_SLOTS = 2048
KPP = 8
CAP = 256
CAPK = 64
N_GX = 64
N_GY = 4
DEVICES = 256


def layout(base):
    seeded = jax.random.fold_in(base, 7)
    first, second, third = jax.random.split(seeded, 3)
    owner_perm = jax.vmap(lambda keyone: jax.random.permutation(keyone, KEY_DEV))(jax.random.split(first, DEVICES))
    device = jnp.arange(DEVICES, dtype=jnp.int32)
    along_x = device // N_GY
    along_y = device % N_GY
    owners = owner_perm // KPP
    within = owner_perm % KPP
    shuffle = jax.vmap(lambda keyone: jax.random.permutation(keyone, KEY_DEV))(jax.random.split(second, N_GX * N_GY))
    shuffle = shuffle.reshape(N_GX, N_GY, KEY_DEV)
    position = shuffle[owners, along_y[:, None], along_x[:, None] * KPP + within]
    key_slot = ((owners * N_GY + along_y[:, None]) * KEY_DEV + position).reshape(KEYS).astype(jnp.int32)
    picked = jax.vmap(lambda keyone: jax.random.permutation(keyone, KEY_DEV)[:HPD])(jax.random.split(third, DEVICES))
    heavy_keys = (device[:, None] * KEY_DEV + picked).reshape(HEAVY).astype(jnp.int32)
    slot_to_key = jnp.argsort(key_slot).astype(jnp.int32)
    heavy_flag = jnp.zeros((KEYS,), jnp.int32).at[heavy_keys].set(1)
    heavy_slot = heavy_flag[slot_to_key]
    return (key_slot, heavy_keys, slot_to_key, heavy_slot)


def draw_key_slot(key, part):
    return layout(key)[0]


def draw_heavy_keys(key, part):
    return layout(key)[1]


def draw_row_keys(key, part):
    key_slot, heavy_keys, slot_to_key, heavy_slot = layout(key)
    seeded = jax.random.fold_in(key, 11)
    favored_pool = jax.random.permutation(jax.random.fold_in(seeded, 3), N_GX)[:max(1, N_GX // 16)]
    tickets = N_GX * CAP
    pool_rank = jnp.where(heavy_slot.reshape(N_GX, OWN_SLOTS) == 1, OWN_SLOTS, 0)

    def one_device(keyone):
        parts = jax.random.split(keyone, 7)
        heavy_count = jax.random.randint(parts[0], (), ROWS_DEV // 4, ROWS_DEV // 2 + 1)
        light_count = ROWS_DEV - heavy_count
        favored = favored_pool[jax.random.randint(parts[1], (), 0, favored_pool.shape[0])]
        ticket_owner = jnp.arange(tickets, dtype=jnp.int32) // CAP
        scores = jnp.where(ticket_owner == favored, 0, tickets) + jax.random.permutation(parts[2], tickets)
        ticket_order = jnp.argsort(scores).astype(jnp.int32)
        row_index = jnp.arange(ROWS_DEV, dtype=jnp.int32)
        chosen = ticket_order[jnp.minimum(row_index, tickets - 1)]
        row_owner = chosen // CAP
        row_ticket = chosen % CAP
        mixing = jax.vmap(lambda keytwo: jax.random.permutation(keytwo, OWN_SLOTS))(jax.random.split(parts[3], N_GX))
        pools = jnp.argsort(pool_rank + mixing, axis=1)[:, :CAPK].astype(jnp.int32)
        spare = jax.random.randint(parts[4], (ROWS_DEV,), 0, CAPK)
        pool_index = jnp.where(row_ticket < CAPK, row_ticket, spare)
        light_keys = slot_to_key[row_owner * OWN_SLOTS + pools[row_owner, pool_index]]
        heavy_pick = heavy_keys[jax.random.randint(parts[5], (ROWS_DEV,), 0, HEAVY)]
        chosen_keys = jnp.where(row_index < light_count, light_keys, heavy_pick)
        return chosen_keys[jax.random.permutation(parts[6], ROWS_DEV)]
    return jax.vmap(one_device)(jax.random.split(seeded, DEVICES)).reshape(ROWS).astype(jnp.int32)


def level_of(own_key, dims, cuts, least, largest):
    factor_of = 1.0
    for dim, shards_of in cuts:
        draws = jax.random.uniform(jax.random.fold_in(jax.random.fold_in(own_key, 6), dim), (shards_of,), jnp.float32, least / len(cuts), largest / len(cuts))
        factor_of = factor_of * jnp.repeat(jnp.exp(draws), dims[dim] // shards_of).reshape((-1,) + (1,) * (len(dims) - 1 - dim))
    return factor_of


def scatter_about(rng, dims, spread, reach, pieces=(), kind=jnp.bfloat16):
    gain = level_of(rng, dims, pieces, -0.22, 0.18) if pieces else 1.0
    drawn = jax.random.normal(rng, dims, jnp.float32) * spread * gain
    return jnp.minimum(jnp.maximum(drawn, -reach), reach).astype(kind)


def setup_inputs(seed: int = 0) -> dict:
    key_list = jax.random.split(jax.random.key(seed), 6)
    return {
        "measures": scatter_about(key_list[0], (ROWS, W), 1.0, 6.0, ((0, 256),)),
        "row_keys": draw_row_keys(jax.random.fold_in(key_list[5], 71), 0),
        "orders": scatter_about(key_list[2], (KEYS, W), 1.0, 6.0, ((0, 256),)),
        "heavy_keys": draw_heavy_keys(jax.random.fold_in(key_list[5], 71), 0),
        "key_slot": draw_key_slot(jax.random.fold_in(key_list[5], 71), 0),
    }


def reference(measures, row_keys, orders, heavy_keys, key_slot):
    blocks = measures.reshape(DEVICES, ROWS_DEV, W)
    block_keys = row_keys.reshape(DEVICES, ROWS_DEV)

    def add_block(running, block_piece):
        block_rows, keys_here = block_piece
        totals = running[0] + jax.ops.segment_sum(block_rows.astype(jnp.float32), keys_here, num_segments=KEYS)
        tallies = running[1] + jax.ops.segment_sum(jnp.ones((ROWS_DEV,), jnp.float32), keys_here, num_segments=KEYS)
        return ((totals, tallies), None)
    start_state = (jnp.zeros((KEYS, W), jnp.float32), jnp.zeros((KEYS,), jnp.float32))
    (sums, counts), unused = lax.scan(add_block, start_state, (blocks, block_keys))
    joined = orders.astype(jnp.float32) * sums * lax.rsqrt(1.0 + counts)[:, None]
    result = joined.astype(jnp.bfloat16)
    heavy_report = joined[heavy_keys].astype(jnp.bfloat16)
    heavy_flag = jnp.zeros((KEYS,), jnp.float32).at[heavy_keys].set(1.0)
    slot_rows = jnp.zeros((KEYS,), jnp.float32).at[key_slot].set(counts * (1.0 - heavy_flag))
    return (result, heavy_report, slot_rows)
```

```python
import jax
import jax.numpy as jnp
from jax import lax
from jax.experimental import pallas as pl
from jax.experimental.pallas import tpu as pltpu
from jax.sharding import PartitionSpec as P

F32, BF16, I16, I32 = jnp.float32, jnp.bfloat16, jnp.int16, jnp.int32
LANES = 128
CODE = 32767.0
TINY = 1e-37


def iota(shape, dim, dtype=I32):
    return lax.broadcasted_iota(dtype, shape, dim)


def packed(index):
    return jnp.concatenate([index, index], axis=0).astype(I16)


def hot(count, index):
    n = index.shape[1]
    label = iota((count, n), 0, I16).reshape(count // 16, 16, n)
    return jnp.where(label == index[None], BF16(1), BF16(0)).reshape(count, n)


def mm(a, b):
    return lax.dot_general(a, b, (((1,), (0,)), ((), ())), preferred_element_type=F32)


def mm_nt(a, b):
    return lax.dot_general(a, b, (((1,), (1,)), ((), ())), preferred_element_type=F32)


def flag(mask):
    return jnp.where(mask, 1.0, 0.0).astype(BF16)


def picked(table, index):
    n = index.shape[1]
    hit = iota((LANES, n), 0).reshape(LANES // 8, 8, n) == index[None]
    part = jnp.sum(jnp.where(hit, table.reshape(LANES // 8, 8, n), 0.0), axis=0)
    return jnp.broadcast_to(jnp.sum(part, axis=0, keepdims=True), (8, n))


def exponent(top):
    return jnp.ceil(jnp.log2(jnp.maximum(top, TINY))) + 1.0


def coded(x, shrink):
    y = jnp.sqrt(jnp.sqrt(jnp.abs(x) * shrink)) * CODE + 0.5
    return jnp.where(x < 0, -y, y)


def decoded(code, stretch):
    t = code.astype(F32) * (1.0 / CODE)
    s = t * t
    return s * s * jnp.where(t < 0, -stretch, stretch)


def split2(x):
    high = x.astype(BF16)
    return high, (x - high.astype(F32)).astype(BF16)


def pack_kernel(
    keys_ref, slots_ref, heavy_ref, rows_hbm, out_ref, rows, table, slot_s, place_s, half_s, count_s, meta_s, masked, sem
):
    row_count = rows.shape[0]
    step = 1024
    tiles = step // LANES
    steps = row_count // step
    copy = pltpu.make_async_copy(rows_hbm, rows, sem)
    copy.start()

    slots_t = slots_ref[...].T
    hk = jnp.concatenate([heavy_ref[i : i + 1, :] for i in range(4)], axis=1)
    hk = jnp.broadcast_to(hk, (8, 512))
    weight = (1 + (iota((LANES, 512), 1) & 1)).astype(BF16)
    marks = mm_nt(hot(LANES, packed(hk & 127)) * weight, hot(1024, packed(hk >> 7)))
    table[0:LANES, :] = jnp.where(marks > 0, -marks, (slots_t >> 9).astype(F32)).astype(BF16)
    table[LANES:, :] = jnp.where(marks > 0, 0.0, ((slots_t & 511) - 256).astype(F32)).astype(BF16)
    count_s[...] = jnp.zeros_like(count_s)

    def look_up(t, carry):
        block = keys_ref[pl.ds(t * tiles, tiles), :]
        key = jnp.concatenate([jnp.broadcast_to(block[i : i + 1, :], (8, LANES)) for i in range(tiles)], axis=1)
        found = mm(table[...], hot(1024, packed(key >> 7)))
        high = picked(found[:LANES], key & 127).astype(I32)
        low = picked(found[LANES:], key & 127).astype(I32)
        heavy = high < 0
        slot = jnp.where(heavy, -1 - (2 * (key >> 9) - 1 - high), high * 512 + low + 256)
        slot_s[:, pl.ds(t * step, step)] = slot
        major = jnp.where(heavy, -1, (slot >> 7) & 511)
        minor = ((slot >> 16) & 1) * LANES + (slot & 127)
        count_s[...] += mm_nt(hot(512, packed(major)), hot(256, packed(minor)))
        return carry

    lax.fori_loop(0, steps, look_up, 0)

    present = flag(count_s[...] > 0)
    a, b = iota((256, 512), 0), iota((256, 512), 1)
    b_in = b & 255
    same_half = (a >> 7) == (b_in >> 7)
    both = mm(present, flag(same_half & ((b >= 256) | (a < b_in))))
    a, b = iota((512, 512), 0), iota((512, 512), 1)
    earlier = flag((b < a) & ((a >> 4) == (b >> 4)))
    rank = both[:, :256] + mm(earlier, both[:, 256:].astype(BF16))
    table[0:LANES, 0:512] = rank[:, :LANES].T.astype(BF16)
    table[0:LANES, 512:1024] = rank[:, LANES:].T.astype(BF16)
    meta_s[...] = jnp.zeros_like(meta_s)

    def place(t, carry):
        slot = slot_s[:, pl.ds(t * step, step)]
        light = slot >= 0
        found = mm(table[0:LANES, :], hot(1024, packed(slot >> 7)))
        rank_here = picked(found, slot & 127).astype(I32)
        owner = slot >> 11
        heavy_id = -1 - slot
        at = jnp.where(light, (owner & 31) * 64 + rank_here, 2048 + (heavy_id & 255))
        place_s[:, pl.ds(t * step, step)] = packed(at)
        half = jnp.where(light, owner >> 5, heavy_id >> 8).astype(F32)
        rows_of = jnp.zeros((tiles, LANES), F32)
        for i in range(tiles):
            rows_of = jnp.where(iota((tiles, LANES), 0) == i, half[:, i * LANES : (i + 1) * LANES], rows_of)
        half_s[pl.ds(t * tiles, tiles), :] = rows_of
        owners = hot(64, packed(jnp.where(light, owner, -1)))
        inside = slot & 2047
        high = jnp.broadcast_to((inside >> 6).astype(F32)[0:1], (64, step)).astype(BF16)
        low = jnp.broadcast_to((inside & 63).astype(F32)[0:1], (64, step)).astype(BF16)
        left = jnp.concatenate(
            [owners, owners * high, owners * low, hot(16, packed(jnp.where(light, -1, heavy_id >> 5)))], axis=0
        )
        right = hot(LANES, packed(jnp.where(light, rank_here, 64 + (heavy_id & 31))))
        meta_s[...] += mm_nt(left, right)
        return carry

    lax.fori_loop(0, steps, place, 0)

    copy.wait()
    top = jnp.zeros((16, LANES), BF16)
    for i in range(row_count // 1024):
        piece = jnp.abs(rows[i * 1024 : (i + 1) * 1024, :]).reshape(64, 16, LANES)
        top = jnp.maximum(top, jnp.max(piece, axis=0))
    power = exponent(jnp.max(jnp.max(top.astype(F32), axis=0, keepdims=True), axis=1, keepdims=True))
    shrink_light = jnp.exp2(-8.0 - power)
    shrink_heavy = jnp.exp2(-13.0 - power)
    lane = iota((64, LANES), 1)
    number = meta_s[0:64, :]
    inside = jnp.where(
        number > 0,
        jnp.round(meta_s[64:128, :] / jnp.maximum(number, 1.0)) * 64.0
        + jnp.round(meta_s[128:192, :] / jnp.maximum(number, 1.0)),
        -1.0,
    )
    first = jnp.where(lane < 64, inside, pltpu.roll(number, 64, 1))
    groups = meta_s[192:208, :]
    spread = jnp.concatenate([jnp.broadcast_to(groups[i : i + 1, :], (4, LANES)) for i in range(16)], axis=0)
    owner_row = iota((64, LANES), 0)
    moved = jnp.zeros((64, LANES), F32)
    for c in range(4):
        moved = jnp.where((owner_row & 3) == c, pltpu.roll(spread, 64 - 8 * c, 1), moved)
    moved_high = jnp.floor(moved * (1.0 / 128.0))
    moved_low = moved - 128.0 * moved_high
    second = jnp.where(lane < 8, moved_low, jnp.where(lane < 16, pltpu.roll(moved_high, 8, 1), power))

    half_t = half_s[...].T
    for i in range(row_count // LANES):
        mine = jnp.broadcast_to(half_t[:, i : i + 1], (LANES, LANES)) > 0
        piece = rows[i * LANES : (i + 1) * LANES, :].astype(F32)
        masked[i * LANES : (i + 1) * LANES, 0:LANES] = jnp.where(mine, 0.0, piece).astype(BF16)
        masked[i * LANES : (i + 1) * LANES, LANES:] = jnp.where(mine, piece, 0.0).astype(BF16)

    def block_sums(b):
        total = jnp.zeros((256, 256), F32)
        for c in range(row_count // 2048):
            index = place_s[:, c * 2048 : (c + 1) * 2048] - (b * 256).astype(I16)
            total += mm(hot(256, index), masked[c * 2048 : (c + 1) * 2048, :])
        return total

    def light_block(b, carry):
        total = coded(block_sums(b), shrink_light)
        for h in range(2):
            piece = total[:, h * LANES : (h + 1) * LANES].astype(I32).astype(I16).reshape(4, 64, LANES)
            out_ref[pl.ds(h * 32 + b * 4, 4), 0:64, :] = piece
        return carry

    lax.fori_loop(0, 8, light_block, 0)
    total = coded(block_sums(jnp.int32(8)), shrink_heavy)
    sub = iota((32, 8, LANES), 1)
    for h in range(2):
        own = slice(h * 32, h * 32 + 32)
        sums = total[:, h * LANES : (h + 1) * LANES].reshape(32, 8, LANES)
        extra = jnp.where(sub == 0, first[own][:, None, :], jnp.where(sub == 1, second[own][:, None, :], 0.0))
        out_ref[own, 64:80, :] = jnp.concatenate([sums, extra], axis=1).astype(I32).astype(I16)


def pack(row_keys, key_slot, heavy_keys, measures):
    n = measures.shape[0]
    return pl.pallas_call(
        pack_kernel,
        out_shape=jax.ShapeDtypeStruct((64, 80, LANES), I16),
        in_specs=[pl.BlockSpec(memory_space=pltpu.VMEM)] * 3 + [pl.BlockSpec(memory_space=pl.ANY)],
        scratch_shapes=[
            pltpu.VMEM((n, LANES), BF16),
            pltpu.VMEM((256, 1024), BF16),
            pltpu.VMEM((8, n), I32),
            pltpu.VMEM((16, n), I16),
            pltpu.VMEM((n // LANES, LANES), F32),
            pltpu.VMEM((512, 256), F32),
            pltpu.VMEM((208, LANES), F32),
            pltpu.VMEM((n, 256), BF16),
            pltpu.SemaphoreType.DMA,
        ],
        compiler_params=pltpu.CompilerParams(vmem_limit_bytes=56 * 2**20),
        name="pack",
    )(row_keys.reshape(-1, LANES), key_slot.reshape(-1, LANES), heavy_keys.reshape(-1, LANES), measures)


def label_kernel(me_ref, slots_ref, out_ref):
    slots = slots_ref[...]
    mine = (slots >> 11) == me_ref[0]
    inside = (slots & 2047).astype(F32)
    a, b = iota((LANES, 256), 0), iota((LANES, 256), 1)
    both = mm(flag(mine), flag((b >= LANES) | (a < b)))
    a, b = iota((256, 256), 0), iota((256, 256), 1)
    earlier = flag((b < a) & ((a >> 2) == (b >> 2)))
    lane = iota((256, LANES), 1)
    rows = []
    for c in range(4):
        part = slice(c * 256, (c + 1) * 256)
        rank = both[part, :LANES] + mm(earlier, both[part, LANES:].astype(BF16))
        found = jnp.zeros((256, LANES), F32)
        for j in range(8):
            value = jnp.where(mine[part] & (rank == float(j)), inside[part], 0.0)
            found = jnp.where(lane == j, jnp.sum(value, axis=1, keepdims=True), found)
        rows.append(jnp.sum(found.reshape(64, 4, LANES), axis=1))
    out_ref[...] = jnp.concatenate(rows, axis=0)


def labels_of(index_x, key_slot):
    order = key_slot.reshape(64, 4, 4, LANES).transpose(1, 0, 2, 3).reshape(1024, LANES)
    return pl.pallas_call(
        label_kernel,
        out_shape=jax.ShapeDtypeStruct((256, LANES), F32),
        in_specs=[pl.BlockSpec(memory_space=pltpu.SMEM), pl.BlockSpec(memory_space=pltpu.VMEM)],
        name="labels",
    )(index_x.reshape(1), order)


def owner_kernel(got_ref, label_ref, out_ref, pair_s, index_s, weight_s, sums_s):
    sources = got_ref.shape[0]
    lane = iota((sources, LANES), 1)
    tail = got_ref[:, 64:80, :].astype(F32)
    first = tail[:, 8, :]
    second = tail[:, 9, :]
    stretch = jnp.exp2(tail[:, 9:10, LANES - 1 :] + 8.0)
    heavy = jnp.sum(decoded(tail[:, 0:8, :], stretch * 32.0), axis=0)
    heavy_counts = jnp.sum(second, axis=0, keepdims=True)

    swapped = pltpu.roll(first, 64, 1)
    low_lane = iota((1, LANES), 1) < 64
    for i in range(sources // 2):
        even, odd = slice(2 * i, 2 * i + 1), slice(2 * i + 1, 2 * i + 2)
        at = slice(i * LANES, (i + 1) * LANES)
        index = jnp.where(low_lane, first[even], swapped[odd]).astype(I32)
        index_s[:, at] = packed(jnp.broadcast_to(index, (8, LANES)))
        weight = jnp.where(low_lane, swapped[even], first[odd])
        weight_s[:, at] = jnp.broadcast_to(weight, (16, LANES)).astype(BF16)

    for s in range(0, sources, 8):
        values = decoded(got_ref[s : s + 8, 0:64, :].astype(I32), stretch[s : s + 8]).reshape(512, LANES)
        high, low = split2(values)
        pair_s[s * 64 : (s + 8) * 64, 0:LANES] = high
        pair_s[s * 64 : (s + 8) * 64, LANES:] = low

    index = index_s[...]
    wide = index.astype(I32)[0:8]
    histogram = mm_nt(hot(16, packed(wide >> 7)) * weight_s[...], hot(LANES, packed(wide & 127)))

    top = jnp.max(jnp.abs(heavy), axis=0, keepdims=True)
    for j in range(8):
        column = jnp.broadcast_to(label_ref[:, j : j + 1], (256, LANES)).astype(I32).astype(I16)
        column = column.reshape(16, 16, LANES)
        total = jnp.zeros((256, 256), F32)
        for c in range(0, sources * 64, 1024):
            hots = jnp.concatenate(
                [
                    jnp.where(column == index_s[:, c + i * LANES : c + (i + 1) * LANES][None], BF16(1), BF16(0)).reshape(256, LANES)
                    for i in range(8)
                ],
                axis=1,
            )
            total += mm(hots, pair_s[c : c + 1024, :])
        total = total[:, :LANES] + total[:, LANES:]
        sums_s[j] = total
        top = jnp.maximum(top, jnp.max(jnp.abs(total), axis=0, keepdims=True))

    power = exponent(jnp.max(top, axis=1, keepdims=True))
    shrink = jnp.exp2(-power)
    heavy_code = coded(heavy, shrink)
    for q in range(4):
        for j in range(8):
            out_ref[q, j * 64 : (j + 1) * 64, :] = coded(sums_s[j, q * 64 : (q + 1) * 64, :], shrink).astype(I32).astype(I16)
        extra = jnp.concatenate(
            [
                heavy_code[2 * q : 2 * q + 2],
                histogram[4 * q : 4 * q + 4],
                heavy_counts,
                jnp.broadcast_to(power, (1, LANES)),
                jnp.zeros((8, LANES), F32),
            ],
            axis=0,
        )
        out_ref[q, 512:528, :] = extra.astype(I32).astype(I16)


def owner_sums(got, labels):
    return pl.pallas_call(
        owner_kernel,
        out_shape=jax.ShapeDtypeStruct((4, 528, LANES), I16),
        scratch_shapes=[
            pltpu.VMEM((4096, 256), BF16),
            pltpu.VMEM((16, 4096), I16),
            pltpu.VMEM((16, 4096), BF16),
            pltpu.VMEM((8, 256, LANES), F32),
        ],
        compiler_params=pltpu.CompilerParams(vmem_limit_bytes=56 * 2**20),
        name="owner",
    )(got, labels)


def quarter_kernel(me_ref, got_ref, label_ref, out_ref, rows_ref, own_ref, place_s):
    tail = got_ref[:, 512:528, :].astype(F32)
    stretch = jnp.exp2(tail[:, 7:8, :])
    counts = jnp.sum(tail[:, 2:6, :], axis=0)
    rows_ref[...] = counts
    heavy = jnp.sum(decoded(tail[:, 0:2, :], stretch), axis=0)
    heavy_counts = jnp.sum(tail[:, 6, :], axis=0, keepdims=True)
    own_ref[...] = jnp.concatenate([heavy, heavy_counts, jnp.zeros((5, LANES), F32)], axis=0)

    labels = label_ref[pl.ds(me_ref[0] * 64, 64), :].astype(I32)
    lane = iota((64, LANES), 1)
    found = jnp.zeros((64, LANES), F32)
    top = jnp.zeros((1, LANES), F32)
    for j in range(8):
        total = jnp.zeros((64, LANES), F32)
        for s in range(4):
            total += decoded(got_ref[s, j * 64 : (j + 1) * 64, :].astype(I32), stretch[s])
        place_s[:, j, :] = total
        top = jnp.maximum(top, jnp.max(jnp.abs(total), axis=0, keepdims=True))
        column = jnp.broadcast_to(labels[:, j : j + 1], (64, LANES))
        number = jnp.zeros((64, LANES), F32)
        for i in range(4):
            number += jnp.where(column == lane + i * LANES + 512 * me_ref[0], counts[i : i + 1, :], 0.0)
        found = jnp.where(lane == j, jnp.sum(number, axis=1, keepdims=True), found)

    power = exponent(jnp.max(top, axis=1, keepdims=True))
    high = jnp.floor(found * (1.0 / 128.0))
    low = found - 128.0 * high
    line = jnp.where(lane < 8, low, jnp.where(lane < 16, pltpu.roll(high, 8, 1), jnp.broadcast_to(power, (64, LANES))))
    extra = jnp.where(iota((64, 8, LANES), 1) == 0, line[:, None, :], 0.0)
    codes = coded(place_s[...], jnp.exp2(-power)[:, None, :])
    out_ref[...] = jnp.concatenate([codes, extra], axis=1).astype(I32).astype(I16)


def quarter_sums(index_y, got, labels):
    vmem = pl.BlockSpec(memory_space=pltpu.VMEM)
    return pl.pallas_call(
        quarter_kernel,
        out_shape=(
            jax.ShapeDtypeStruct((64, 16, LANES), I16),
            jax.ShapeDtypeStruct((4, LANES), F32),
            jax.ShapeDtypeStruct((8, LANES), F32),
        ),
        in_specs=[pl.BlockSpec(memory_space=pltpu.SMEM), vmem, vmem],
        scratch_shapes=[pltpu.VMEM((64, 8, LANES), F32)],
        name="quarter",
    )(index_y.reshape(1), got, labels)


def join_kernel(heavy_ref, me_ref, got_ref, own_ref, slots_ref, orders_ref, out_ref, report_ref, joined_s):
    block = got_ref[...].astype(F32)
    sums = decoded(block[:, 0:8, :], jnp.exp2(block[:, 8:9, LANES - 1 :])).reshape(512, LANES)
    lane = iota((64, 8, LANES), 2)
    sub = iota((64, 8, LANES), 1)
    line = jnp.broadcast_to(block[:, 8:9, :], (64, 8, LANES))
    low = jnp.sum(jnp.where(lane == sub, line, 0.0), axis=2, keepdims=True)
    high = jnp.sum(jnp.where(lane == sub + 8, line, 0.0), axis=2, keepdims=True)
    low = jnp.broadcast_to(low, (64, 8, LANES)).reshape(512, LANES).astype(BF16)
    high = jnp.broadcast_to(high * 128.0, (64, 8, LANES)).reshape(512, LANES)
    high_a, high_b = split2(high)
    sum_a, sum_b = split2(sums)
    right = jnp.concatenate([sum_a, sum_b, low, high_a, high_b], axis=1)

    owner = slots_ref[...] >> 11
    wide = jnp.concatenate([jnp.broadcast_to(owner[i : i + 1, :], (8, LANES)) for i in range(4)], axis=1)
    padded = jnp.concatenate([owner, owner], axis=0)
    turned = padded.astype(F32).T.astype(I32)
    earlier = jnp.zeros((8, 512), F32)
    k = iota((16, 8, 512), 2)
    for i in range(4):
        column = jnp.broadcast_to(turned[:, i : i + 1], (LANES, 512)).reshape(16, 8, 512)
        other = iota((LANES, 512), 0).reshape(16, 8, 512) + i * LANES
        earlier += jnp.sum(jnp.where((column == wide[None]) & (other < k), 1.0, 0.0), axis=0)
    place = (wide * 8).astype(F32) + jnp.sum(earlier, axis=0, keepdims=True)
    rows = jnp.concatenate([place[0:1, i * LANES : (i + 1) * LANES] for i in range(4)] * 2, axis=0)
    columns = rows.T
    for i in range(4):
        part = slice(i * LANES, (i + 1) * LANES)
        spot = jnp.broadcast_to(columns[:, i : i + 1], (LANES, 512)).astype(I32)
        moved = mm(flag(spot == iota((LANES, 512), 1)), right)
        total = moved[:, 0:LANES] + moved[:, LANES : 2 * LANES]
        number = moved[:, 2 * LANES : 3 * LANES] + (moved[:, 3 * LANES : 4 * LANES] + moved[:, 4 * LANES :])
        key = iota((LANES, LANES), 0) + i * LANES
        for h in range(2):
            hit = key == heavy_ref[h]
            spot = 2 * me_ref[0] + h
            line = own_ref[2:3, :]
            here = iota((1, LANES), 1)
            count = jnp.sum(
                jnp.where(here == spot, line, 0.0) + jnp.where(here == spot + 8, line * 128.0, 0.0), axis=1, keepdims=True
            )
            total = jnp.where(hit, own_ref[h : h + 1, :], total)
            number = jnp.where(hit, count, number)
        joined = orders_ref[part, :].astype(F32) * total * lax.rsqrt(1.0 + number)
        joined_s[part, :] = joined
        out_ref[part, :] = joined.astype(BF16)
    report_ref[...] = jnp.concatenate(
        [joined_s[pl.ds(heavy_ref[0], 1), :], joined_s[pl.ds(heavy_ref[1], 1), :]], axis=0
    ).astype(BF16)


def join(heavy_here, index_y, got, own, slots_here, orders):
    vmem = pl.BlockSpec(memory_space=pltpu.VMEM)
    smem = pl.BlockSpec(memory_space=pltpu.SMEM)
    return pl.pallas_call(
        join_kernel,
        out_shape=(jax.ShapeDtypeStruct((512, LANES), BF16), jax.ShapeDtypeStruct((2, LANES), BF16)),
        in_specs=[smem, smem, vmem, vmem, vmem, vmem],
        scratch_shapes=[pltpu.VMEM((512, LANES), F32)],
        name="join",
    )(heavy_here, index_y.reshape(1), got, own, slots_here, orders)


def body(measures, row_keys, orders, heavy_keys, key_slot):
    index_x = lax.axis_index("gx")
    index_y = lax.axis_index("gy")
    device = index_x * 4 + index_y
    message = pack(row_keys, key_slot, heavy_keys, measures)
    got = lax.all_to_all(message, "gx", split_axis=0, concat_axis=0, tiled=True)
    labels = labels_of(index_x, key_slot)
    partial = owner_sums(got, labels)
    got = lax.all_to_all(partial, "gy", split_axis=0, concat_axis=0, tiled=True)
    message, slot_rows, own = quarter_sums(index_y, got, labels)
    got = lax.all_to_all(message, "gx", split_axis=0, concat_axis=0, tiled=True)
    heavy_here = lax.dynamic_slice_in_dim(heavy_keys, device * 2, 2) - device * 512
    slots_here = lax.dynamic_slice_in_dim(key_slot, device * 512, 512).reshape(4, LANES)
    result, report = join(heavy_here, index_y, got, own, slots_here, orders)
    return result, report, slot_rows.reshape(512)


def solution(mesh):
    return jax.shard_map(
        body,
        mesh=mesh,
        in_specs=(P(("gx", "gy"), None), P(("gx", "gy")), P(("gx", "gy"), None), P(), P()),
        out_specs=(P(("gx", "gy"), None), P(("gx", "gy"), None), P(("gx", "gy"))),
        check_vma=False,
    )
```

```python
import jax
import jax.numpy as jnp
from jax import lax
from jax.experimental import pallas as pl
from jax.experimental.pallas import tpu as pltpu
from jax.sharding import Mesh
from jax.sharding import PartitionSpec as P

F32, BF16, I16, I32 = jnp.float32, jnp.bfloat16, jnp.int16, jnp.int32
LANES = 128
CODE = 32767.0
TINY = 1e-37
AXES = ("x", "t", "low", "core", "y")
GROUP = ("x", "low", "core", "y")


def near(x):
    return pltpu.with_memory_space_constraint(x, pltpu.VMEM)


def iota(shape, dim, dtype=I32):
    return lax.broadcasted_iota(dtype, shape, dim)


def packed(index):
    return jnp.concatenate([index, index], axis=0).astype(I16)


def hot(count, index):
    n = index.shape[1]
    label = iota((count, n), 0, I16).reshape(count // 16, 16, n)
    return jnp.where(label == index[None], BF16(1), BF16(0)).reshape(count, n)


def mm(a, b):
    return lax.dot_general(a, b, (((1,), (0,)), ((), ())), preferred_element_type=F32)


def mm_nt(a, b):
    return lax.dot_general(a, b, (((1,), (1,)), ((), ())), preferred_element_type=F32)


def flag(mask):
    return jnp.where(mask, 1.0, 0.0).astype(BF16)


def picked(table, index):
    n = index.shape[1]
    hit = iota((LANES, n), 0).reshape(LANES // 8, 8, n) == index[None]
    part = jnp.sum(jnp.where(hit, table.reshape(LANES // 8, 8, n), 0.0), axis=0)
    return jnp.broadcast_to(jnp.sum(part, axis=0, keepdims=True), (8, n))


def exponent(top):
    return jnp.ceil(jnp.log2(jnp.maximum(top, TINY))) + 1.0


def coded(x, shrink):
    y = jnp.sqrt(jnp.sqrt(jnp.abs(x) * shrink)) * CODE + 0.5
    return jnp.where(x < 0, -y, y)


def decoded(code, stretch):
    t = code.astype(F32) * (1.0 / CODE)
    s = t * t
    return s * s * jnp.where(t < 0, -stretch, stretch)


def split2(x):
    high = x.astype(BF16)
    return high, (x - high.astype(F32)).astype(BF16)


def peer_of(owner):
    return (owner & 48) | ((owner & 3) << 2) | ((owner >> 2) & 3)


def pack_kernel(
    keys_ref, slots_ref, heavy_ref, rows_hbm, out_ref, rows, table, slot_s, place_s, half_s, count_s, meta_s, masked, sem
):
    row_count = rows.shape[0]
    step = 1024
    tiles = step // LANES
    steps = row_count // step
    copy = pltpu.make_async_copy(rows_hbm, rows, sem)
    copy.start()

    slots_t = slots_ref[...].T
    hk = jnp.concatenate([heavy_ref[i : i + 1, :] for i in range(4)], axis=1)
    hk = jnp.broadcast_to(hk, (8, 512))
    weight = (1 + (iota((LANES, 512), 1) & 1)).astype(BF16)
    marks = mm_nt(hot(LANES, packed(hk & 127)) * weight, hot(1024, packed(hk >> 7)))
    table[0:LANES, :] = jnp.where(marks > 0, -marks, (slots_t >> 9).astype(F32)).astype(BF16)
    table[LANES:, :] = jnp.where(marks > 0, 0.0, ((slots_t & 511) - 256).astype(F32)).astype(BF16)
    count_s[...] = jnp.zeros_like(count_s)

    def look_up(t, carry):
        block = keys_ref[pl.ds(t * tiles, tiles), :]
        key = jnp.concatenate([jnp.broadcast_to(block[i : i + 1, :], (8, LANES)) for i in range(tiles)], axis=1)
        found = mm(table[...], hot(1024, packed(key >> 7)))
        high = picked(found[:LANES], key & 127).astype(I32)
        low = picked(found[LANES:], key & 127).astype(I32)
        heavy = high < 0
        slot = jnp.where(heavy, -1 - (2 * (key >> 9) - 1 - high), high * 512 + low + 256)
        slot_s[:, pl.ds(t * step, step)] = slot
        major = jnp.where(heavy, -1, (slot >> 7) & 511)
        minor = ((slot >> 16) & 1) * LANES + (slot & 127)
        count_s[...] += mm_nt(hot(512, packed(major)), hot(256, packed(minor)))
        return carry

    lax.fori_loop(0, steps, look_up, 0)

    present = flag(count_s[...] > 0)
    a, b = iota((256, 512), 0), iota((256, 512), 1)
    b_in = b & 255
    same_half = (a >> 7) == (b_in >> 7)
    both = mm(present, flag(same_half & ((b >= 256) | (a < b_in))))
    a, b = iota((512, 512), 0), iota((512, 512), 1)
    earlier = flag((b < a) & ((a >> 4) == (b >> 4)))
    rank = both[:, :256] + mm(earlier, both[:, 256:].astype(BF16))
    table[0:LANES, 0:512] = rank[:, :LANES].T.astype(BF16)
    table[0:LANES, 512:1024] = rank[:, LANES:].T.astype(BF16)
    meta_s[...] = jnp.zeros_like(meta_s)

    def place(t, carry):
        slot = slot_s[:, pl.ds(t * step, step)]
        light = slot >= 0
        found = mm(table[0:LANES, :], hot(1024, packed(slot >> 7)))
        rank_here = picked(found, slot & 127).astype(I32)
        owner = slot >> 11
        peer = peer_of(owner)
        heavy_id = -1 - slot
        heavy_peer = peer_of(heavy_id >> 3) & 60 | (heavy_id >> 1) & 3
        heavy_id = heavy_peer * 8 + ((heavy_id >> 5) & 3) * 2 + (heavy_id & 1)
        at = jnp.where(light, (peer & 31) * 64 + rank_here, 2048 + (heavy_id & 255))
        place_s[:, pl.ds(t * step, step)] = packed(at)
        half = jnp.where(light, peer >> 5, heavy_id >> 8).astype(F32)
        rows_of = jnp.zeros((tiles, LANES), F32)
        for i in range(tiles):
            rows_of = jnp.where(iota((tiles, LANES), 0) == i, half[:, i * LANES : (i + 1) * LANES], rows_of)
        half_s[pl.ds(t * tiles, tiles), :] = rows_of
        owners = hot(64, packed(jnp.where(light, peer, -1)))
        inside = slot & 2047
        high = jnp.broadcast_to((inside >> 6).astype(F32)[0:1], (64, step)).astype(BF16)
        low = jnp.broadcast_to((inside & 63).astype(F32)[0:1], (64, step)).astype(BF16)
        left = jnp.concatenate(
            [owners, owners * high, owners * low, hot(16, packed(jnp.where(light, -1, heavy_id >> 5)))], axis=0
        )
        right = hot(LANES, packed(jnp.where(light, rank_here, 64 + (heavy_id & 31))))
        meta_s[...] += mm_nt(left, right)
        return carry

    lax.fori_loop(0, steps, place, 0)

    copy.wait()
    top = jnp.zeros((16, LANES), BF16)
    for i in range(row_count // 1024):
        piece = jnp.abs(rows[i * 1024 : (i + 1) * 1024, :]).reshape(64, 16, LANES)
        top = jnp.maximum(top, jnp.max(piece, axis=0))
    power = exponent(jnp.max(jnp.max(top.astype(F32), axis=0, keepdims=True), axis=1, keepdims=True))
    shrink_light = jnp.exp2(-8.0 - power)
    shrink_heavy = jnp.exp2(-13.0 - power)
    lane = iota((64, LANES), 1)
    number = meta_s[0:64, :]
    inside = jnp.where(
        number > 0,
        jnp.round(meta_s[64:128, :] / jnp.maximum(number, 1.0)) * 64.0
        + jnp.round(meta_s[128:192, :] / jnp.maximum(number, 1.0)),
        -1.0,
    )
    first = jnp.where(lane < 64, inside, pltpu.roll(number, 64, 1))
    groups = meta_s[192:208, :]
    spread = jnp.concatenate([jnp.broadcast_to(groups[i : i + 1, :], (4, LANES)) for i in range(16)], axis=0)
    owner_row = iota((64, LANES), 0)
    moved = jnp.zeros((64, LANES), F32)
    for c in range(4):
        moved = jnp.where((owner_row & 3) == c, pltpu.roll(spread, 64 - 8 * c, 1), moved)
    moved_high = jnp.floor(moved * (1.0 / 128.0))
    moved_low = moved - 128.0 * moved_high
    second = jnp.where(lane < 8, moved_low, jnp.where(lane < 16, pltpu.roll(moved_high, 8, 1), power))

    half_t = half_s[...].T
    for i in range(row_count // LANES):
        mine = jnp.broadcast_to(half_t[:, i : i + 1], (LANES, LANES)) > 0
        piece = rows[i * LANES : (i + 1) * LANES, :].astype(F32)
        masked[i * LANES : (i + 1) * LANES, 0:LANES] = jnp.where(mine, 0.0, piece).astype(BF16)
        masked[i * LANES : (i + 1) * LANES, LANES:] = jnp.where(mine, piece, 0.0).astype(BF16)

    def block_sums(b):
        total = jnp.zeros((256, 256), F32)
        for c in range(row_count // 2048):
            index = place_s[:, c * 2048 : (c + 1) * 2048] - (b * 256).astype(I16)
            total += mm(hot(256, index), masked[c * 2048 : (c + 1) * 2048, :])
        return total

    def light_block(b, carry):
        total = coded(block_sums(b), shrink_light)
        for h in range(2):
            piece = total[:, h * LANES : (h + 1) * LANES].astype(I32).astype(I16).reshape(4, 64, LANES)
            out_ref[pl.ds(h * 32 + b * 4, 4), 0:64, :] = piece
        return carry

    lax.fori_loop(0, 8, light_block, 0)
    total = coded(block_sums(jnp.int32(8)), shrink_heavy)
    sub = iota((32, 8, LANES), 1)
    for h in range(2):
        own = slice(h * 32, h * 32 + 32)
        sums = total[:, h * LANES : (h + 1) * LANES].reshape(32, 8, LANES)
        extra = jnp.where(sub == 0, first[own][:, None, :], jnp.where(sub == 1, second[own][:, None, :], 0.0))
        out_ref[own, 64:80, :] = jnp.concatenate([sums, extra], axis=1).astype(I32).astype(I16)


def pack(row_keys, key_slot, heavy_keys, measures):
    n = measures.shape[0]
    return pl.pallas_call(
        pack_kernel,
        out_shape=pltpu.VMEM((64, 80, LANES), I16),
        in_specs=[pl.BlockSpec(memory_space=pltpu.VMEM)] * 3 + [pl.BlockSpec(memory_space=pl.ANY)],
        scratch_shapes=[
            pltpu.VMEM((n, LANES), BF16),
            pltpu.VMEM((256, 1024), BF16),
            pltpu.VMEM((8, n), I32),
            pltpu.VMEM((16, n), I16),
            pltpu.VMEM((n // LANES, LANES), F32),
            pltpu.VMEM((512, 256), F32),
            pltpu.VMEM((208, LANES), F32),
            pltpu.VMEM((n, 256), BF16),
            pltpu.SemaphoreType.DMA,
        ],
        compiler_params=pltpu.CompilerParams(vmem_limit_bytes=56 * 2**20),
        name="pack",
    )(row_keys.reshape(-1, LANES), key_slot.reshape(-1, LANES), heavy_keys.reshape(-1, LANES), measures)


def label_kernel(me_ref, slots_ref, out_ref):
    slots = slots_ref[...]
    mine = (slots >> 11) == me_ref[0]
    inside = (slots & 2047).astype(F32)
    a, b = iota((LANES, 256), 0), iota((LANES, 256), 1)
    both = mm(flag(mine), flag((b >= LANES) | (a < b)))
    a, b = iota((256, 256), 0), iota((256, 256), 1)
    earlier = flag((b < a) & ((a >> 2) == (b >> 2)))
    lane = iota((256, LANES), 1)
    rows = []
    for c in range(4):
        part = slice(c * 256, (c + 1) * 256)
        rank = both[part, :LANES] + mm(earlier, both[part, LANES:].astype(BF16))
        found = jnp.zeros((256, LANES), F32)
        for j in range(8):
            value = jnp.where(mine[part] & (rank == float(j)), inside[part], 0.0)
            found = jnp.where(lane == j, jnp.sum(value, axis=1, keepdims=True), found)
        rows.append(jnp.sum(found.reshape(64, 4, LANES), axis=1))
    out_ref[...] = jnp.concatenate(rows, axis=0)


def labels_of(owner, key_slot):
    order = key_slot.reshape(4, 4, 16, 4, LANES).transpose(1, 0, 2, 3, 4).reshape(1024, LANES)
    return pl.pallas_call(
        label_kernel,
        out_shape=pltpu.VMEM((256, LANES), F32),
        in_specs=[pl.BlockSpec(memory_space=pltpu.SMEM), pl.BlockSpec(memory_space=pltpu.VMEM)],
        name="labels",
    )(owner.reshape(1), order)


def slot_sums(labels, index_s, pair_s):
    column = jnp.concatenate([jnp.broadcast_to(labels[:, j : j + 1], (64, LANES)) for j in range(8)], axis=0)
    column = column.astype(I32).astype(I16).reshape(32, 16, LANES)
    total = jnp.zeros((512, 256), F32)
    for c in range(0, 4096, 1024):
        hots = jnp.concatenate(
            [
                jnp.where(column == index_s[:, c + i : c + i + LANES][None], BF16(1), BF16(0)).reshape(512, LANES)
                for i in range(0, 1024, LANES)
            ],
            axis=1,
        )
        total += mm(hots, pair_s[c : c + 1024, :])
    return total[:, :LANES] + total[:, LANES:]


def owner_kernel(me_ref, got_ref, label_ref, a_ref, b_ref, c_ref, own_ref, pair_s, index_s, weight_s):
    sources = got_ref.shape[0]
    tail = got_ref[:, 64:80, :].astype(F32)
    first = tail[:, 8, :]
    second = tail[:, 9, :]
    stretch = jnp.exp2(tail[:, 9:10, LANES - 1 :] + 8.0)
    heavy = jnp.sum(decoded(tail[:, 0:8, :], stretch * 32.0), axis=0)
    heavy_counts = jnp.sum(second, axis=0, keepdims=True)

    swapped = pltpu.roll(first, 64, 1)
    low_lane = iota((1, LANES), 1) < 64
    for i in range(sources // 2):
        even, odd = slice(2 * i, 2 * i + 1), slice(2 * i + 1, 2 * i + 2)
        at = slice(i * LANES, (i + 1) * LANES)
        index = jnp.where(low_lane, first[even], swapped[odd]).astype(I32)
        index_s[:, at] = packed(jnp.broadcast_to(index, (8, LANES)))
        weight = jnp.where(low_lane, swapped[even], first[odd])
        weight_s[:, at] = jnp.broadcast_to(weight, (16, LANES)).astype(BF16)

    for s in range(0, sources, 8):
        values = decoded(got_ref[s : s + 8, 0:64, :].astype(I32), stretch[s : s + 8]).reshape(512, LANES)
        high, low = split2(values)
        pair_s[s * 64 : (s + 8) * 64, 0:LANES] = high
        pair_s[s * 64 : (s + 8) * 64, LANES:] = low

    wide = index_s[...].astype(I32)[0:8]
    histogram = mm_nt(hot(16, packed(wide >> 7)) * weight_s[...], hot(LANES, packed(wide & 127)))

    for i, out_ref in enumerate((a_ref, b_ref, c_ref, own_ref)):
        t = (me_ref[0] + 1 + i) & 3
        total = slot_sums(label_ref[pl.ds(t * 64, 64), :], index_s, pair_s)
        heavy_here = heavy[0:2]
        for p in range(1, 4):
            heavy_here = jnp.where(t == p, heavy[2 * p : 2 * p + 2], heavy_here)
        top = jnp.maximum(jnp.max(jnp.abs(total), axis=0, keepdims=True), jnp.max(jnp.abs(heavy_here), axis=0, keepdims=True))
        power = exponent(jnp.max(top, axis=1, keepdims=True))
        shrink = jnp.exp2(-power)
        out_ref[0:512, :] = coded(total, shrink).astype(I32).astype(I16)
        extra = jnp.concatenate(
            [
                histogram,
                coded(heavy_here, shrink),
                heavy_counts,
                jnp.broadcast_to(power, (1, LANES)),
                jnp.zeros((12, LANES), F32),
            ],
            axis=0,
        )
        out_ref[512:544, :] = extra.astype(I32).astype(I16)


def owner_sums(index_t, got, labels):
    vmem = pl.BlockSpec(memory_space=pltpu.VMEM)
    return pl.pallas_call(
        owner_kernel,
        out_shape=(pltpu.VMEM((544, LANES), I16),) * 4,
        in_specs=[pl.BlockSpec(memory_space=pltpu.SMEM), vmem, vmem],
        scratch_shapes=[pltpu.VMEM((4096, 256), BF16), pltpu.VMEM((16, 4096), I16), pltpu.VMEM((16, 4096), BF16)],
        compiler_params=pltpu.CompilerParams(vmem_limit_bytes=32 * 2**20),
        name="owner",
    )(index_t.reshape(1), near(got), near(labels))


def quarter_kernel(me_ref, a_ref, b_ref, c_ref, d_ref, label_ref, out_ref, own_ref, r0_ref, r1_ref, r2_ref, r3_ref, place_s):
    parts = (a_ref, b_ref, c_ref, d_ref)
    tails = [ref[512:544, :].astype(F32) for ref in parts]
    stretch = [jnp.exp2(tail[19:20, :]) for tail in tails]
    counts = sum(tail[0:16, :] for tail in tails)
    heavy = sum(decoded(tail[16:18, :], s) for tail, s in zip(tails, stretch))
    heavy_counts = sum(tail[18:19, :] for tail in tails)
    own_ref[...] = jnp.concatenate([heavy, heavy_counts, jnp.zeros((5, LANES), F32)], axis=0)
    for i, rows_ref in enumerate((r0_ref, r1_ref, r2_ref, r3_ref)):
        q = (me_ref[0] + i) & 3
        rows = counts[0:4]
        for p in range(1, 4):
            rows = jnp.where(q == p, counts[4 * p : 4 * p + 4], rows)
        rows_ref[...] = rows

    labels = label_ref[pl.ds(me_ref[0] * 64, 64), :].astype(I32)
    lane = iota((64, LANES), 1)
    found = jnp.zeros((64, LANES), F32)
    top = jnp.zeros((1, LANES), F32)
    for j in range(8):
        total = jnp.zeros((64, LANES), F32)
        for s in range(4):
            total += decoded(parts[s][j * 64 : (j + 1) * 64, :].astype(I32), stretch[s])
        place_s[:, j, :] = total
        top = jnp.maximum(top, jnp.max(jnp.abs(total), axis=0, keepdims=True))
        column = jnp.broadcast_to(labels[:, j : j + 1], (64, LANES))
        number = jnp.zeros((64, LANES), F32)
        for i in range(16):
            number += jnp.where(column == lane + i * LANES, counts[i : i + 1, :], 0.0)
        found = jnp.where(lane == j, jnp.sum(number, axis=1, keepdims=True), found)

    power = exponent(jnp.max(top, axis=1, keepdims=True))
    high = jnp.floor(found * (1.0 / 128.0))
    low = found - 128.0 * high
    line = jnp.where(lane < 8, low, jnp.where(lane < 16, pltpu.roll(high, 8, 1), jnp.broadcast_to(power, (64, LANES))))
    extra = jnp.where(iota((64, 8, LANES), 1) == 0, line[:, None, :], 0.0)
    codes = coded(place_s[...], jnp.exp2(-power)[:, None, :])
    out_ref[...] = jnp.concatenate([codes, extra], axis=1).astype(I32).astype(I16)


def quarter_sums(index_t, parts, labels):
    vmem = pl.BlockSpec(memory_space=pltpu.VMEM)
    return pl.pallas_call(
        quarter_kernel,
        out_shape=(pltpu.VMEM((64, 16, LANES), I16), pltpu.VMEM((8, LANES), F32))
        + (jax.ShapeDtypeStruct((4, LANES), F32),) * 4,
        in_specs=[pl.BlockSpec(memory_space=pltpu.SMEM)] + [vmem] * 5,
        scratch_shapes=[pltpu.VMEM((64, 8, LANES), F32)],
        name="quarter",
    )(index_t.reshape(1), *[near(part) for part in parts], near(labels))


def join_kernel(heavy_ref, me_ref, got_ref, own_ref, slots_ref, orders_ref, out_ref, report_ref, joined_s):
    block = got_ref[...].astype(F32)
    sums = decoded(block[:, 0:8, :], jnp.exp2(block[:, 8:9, LANES - 1 :])).reshape(512, LANES)
    lane = iota((64, 8, LANES), 2)
    sub = iota((64, 8, LANES), 1)
    line = jnp.broadcast_to(block[:, 8:9, :], (64, 8, LANES))
    low = jnp.sum(jnp.where(lane == sub, line, 0.0), axis=2, keepdims=True)
    high = jnp.sum(jnp.where(lane == sub + 8, line, 0.0), axis=2, keepdims=True)
    low = jnp.broadcast_to(low, (64, 8, LANES)).reshape(512, LANES).astype(BF16)
    high = jnp.broadcast_to(high * 128.0, (64, 8, LANES)).reshape(512, LANES)
    high_a, high_b = split2(high)
    sum_a, sum_b = split2(sums)
    right = jnp.concatenate([sum_a, sum_b, low, high_a, high_b], axis=1)

    owner = peer_of(slots_ref[...] >> 11)
    wide = jnp.concatenate([jnp.broadcast_to(owner[i : i + 1, :], (8, LANES)) for i in range(4)], axis=1)
    padded = jnp.concatenate([owner, owner], axis=0)
    turned = padded.astype(F32).T.astype(I32)
    earlier = jnp.zeros((8, 512), F32)
    k = iota((16, 8, 512), 2)
    for i in range(4):
        column = jnp.broadcast_to(turned[:, i : i + 1], (LANES, 512)).reshape(16, 8, 512)
        other = iota((LANES, 512), 0).reshape(16, 8, 512) + i * LANES
        earlier += jnp.sum(jnp.where((column == wide[None]) & (other < k), 1.0, 0.0), axis=0)
    place = (wide * 8).astype(F32) + jnp.sum(earlier, axis=0, keepdims=True)
    rows = jnp.concatenate([place[0:1, i * LANES : (i + 1) * LANES] for i in range(4)] * 2, axis=0)
    columns = rows.T
    for i in range(4):
        part = slice(i * LANES, (i + 1) * LANES)
        spot = jnp.broadcast_to(columns[:, i : i + 1], (LANES, 512)).astype(I32)
        moved = mm(flag(spot == iota((LANES, 512), 1)), right)
        total = moved[:, 0:LANES] + moved[:, LANES : 2 * LANES]
        number = moved[:, 2 * LANES : 3 * LANES] + (moved[:, 3 * LANES : 4 * LANES] + moved[:, 4 * LANES :])
        key = iota((LANES, LANES), 0) + i * LANES
        for h in range(2):
            hit = key == heavy_ref[h]
            spot = 2 * me_ref[0] + h
            line = own_ref[2:3, :]
            here = iota((1, LANES), 1)
            count = jnp.sum(
                jnp.where(here == spot, line, 0.0) + jnp.where(here == spot + 8, line * 128.0, 0.0), axis=1, keepdims=True
            )
            total = jnp.where(hit, own_ref[h : h + 1, :], total)
            number = jnp.where(hit, count, number)
        joined = orders_ref[part, :].astype(F32) * total * lax.rsqrt(1.0 + number)
        joined_s[part, :] = joined
        out_ref[part, :] = joined.astype(BF16)
    report_ref[...] = jnp.concatenate(
        [joined_s[pl.ds(heavy_ref[0], 1), :], joined_s[pl.ds(heavy_ref[1], 1), :]], axis=0
    ).astype(BF16)


def join(heavy_here, index_y, got, own, slots_here, orders):
    vmem = pl.BlockSpec(memory_space=pltpu.VMEM)
    smem = pl.BlockSpec(memory_space=pltpu.SMEM)
    return pl.pallas_call(
        join_kernel,
        out_shape=(jax.ShapeDtypeStruct((512, LANES), BF16), jax.ShapeDtypeStruct((2, LANES), BF16)),
        in_specs=[smem, smem, vmem, vmem, vmem, vmem],
        scratch_shapes=[pltpu.VMEM((512, LANES), F32)],
        name="join",
    )(heavy_here, index_y.reshape(1), near(got), near(own), slots_here, orders)


def swap(x):
    return lax.all_to_all(x, GROUP, split_axis=0, concat_axis=0, tiled=True)


def body(measures, row_keys, orders, heavy_keys, key_slot):
    x, t, low, core, y = (lax.axis_index(name) for name in AXES)
    device = (((x * 4 + t) * 2 + low) * 2 + core) * 4 + y
    owner = ((x * 4 + y) * 2 + low) * 2 + core
    got = swap(pack(row_keys, key_slot, heavy_keys, measures))
    labels = labels_of(owner, key_slot)
    *sent, kept = owner_sums(t, got, labels)
    parts = [lax.ppermute(part, "t", [(s, (s + 1 + i) % 4) for s in range(4)]) for i, part in enumerate(sent)]
    message, own, *rows = quarter_sums(t, parts + [kept], labels)
    got = swap(message)
    slot_rows = jnp.where(y == t, rows[0], 0.0)
    for i in range(1, 4):
        slot_rows += lax.ppermute(rows[i], ("t", "y"), [(5 * s, 4 * s + (s + i) % 4) for s in range(4)])
    heavy_here = lax.dynamic_slice_in_dim(heavy_keys, device * 2, 2) - device * 512
    slots_here = lax.dynamic_slice_in_dim(key_slot, device * 512, 512).reshape(4, LANES)
    result, report = join(heavy_here, t, got, own, slots_here, orders)
    return result, report, slot_rows.reshape(512)


def solution(mesh):
    split = Mesh(mesh.devices.reshape(4, 4, 2, 2, 4), AXES)
    return jax.shard_map(
        body,
        mesh=split,
        in_specs=(P(AXES, None), P(AXES), P(AXES, None), P(), P()),
        out_specs=(P(AXES, None), P(AXES, None), P(AXES)),
        check_vma=False,
    )
```

```python
import jax
import jax.numpy as jnp
from jax import lax
from jax.experimental import pallas as pl
from jax.experimental.pallas import tpu as pltpu
from jax.sharding import Mesh
from jax.sharding import PartitionSpec as P

F32, BF16, I16, I32 = jnp.float32, jnp.bfloat16, jnp.int16, jnp.int32
LANES = 128
CODE = 32767.0
TINY = 1e-37
AXES = ("x", "t", "low", "core", "y")
GROUP = ("x", "low", "core", "y")


def near(x):
    return pltpu.with_memory_space_constraint(x, pltpu.VMEM)


def iota(shape, dim, dtype=I32):
    return lax.broadcasted_iota(dtype, shape, dim)


def packed(index):
    return jnp.concatenate([index, index], axis=0).astype(I16)


def hot(count, index):
    n = index.shape[1]
    label = iota((count, n), 0, I16).reshape(count // 16, 16, n)
    return jnp.where(label == index[None], BF16(1), BF16(0)).reshape(count, n)


def mm(a, b):
    return lax.dot_general(a, b, (((1,), (0,)), ((), ())), preferred_element_type=F32)


def mm_nt(a, b):
    return lax.dot_general(a, b, (((1,), (1,)), ((), ())), preferred_element_type=F32)


def flag(mask):
    return jnp.where(mask, 1.0, 0.0).astype(BF16)


def picked(table, index):
    n = index.shape[1]
    hit = iota((LANES, n), 0).reshape(LANES // 8, 8, n) == index[None]
    part = jnp.sum(jnp.where(hit, table.reshape(LANES // 8, 8, n), 0.0), axis=0)
    return jnp.broadcast_to(jnp.sum(part, axis=0, keepdims=True), (8, n))


def exponent(top):
    return jnp.ceil(jnp.log2(jnp.maximum(top, TINY))) + 1.0


def coded(x, shrink):
    y = jnp.sqrt(jnp.sqrt(jnp.abs(x) * shrink)) * CODE + 0.5
    return jnp.where(x < 0, -y, y)


def decoded(code, stretch):
    t = code.astype(F32) * (1.0 / CODE)
    s = t * t
    return s * s * jnp.where(t < 0, -stretch, stretch)


def split2(x):
    high = x.astype(BF16)
    return high, (x - high.astype(F32)).astype(BF16)


def peer_of(owner):
    return (owner & 48) | ((owner & 3) << 2) | ((owner >> 2) & 3)


def pack_kernel(
    keys_ref, slots_ref, heavy_ref, rows_hbm, out_ref, rows, table, slot_s, place_s, half_s, count_s, meta_s, masked, sem
):
    row_count = rows.shape[0]
    step = 1024
    tiles = step // LANES
    steps = row_count // step
    copy = pltpu.make_async_copy(rows_hbm, rows, sem)
    copy.start()

    slots_t = slots_ref[...].T
    hk = jnp.concatenate([heavy_ref[i : i + 1, :] for i in range(4)], axis=1)
    hk = jnp.broadcast_to(hk, (8, 512))
    weight = (1 + (iota((LANES, 512), 1) & 1)).astype(BF16)
    marks = mm_nt(hot(LANES, packed(hk & 127)) * weight, hot(1024, packed(hk >> 7)))
    table[0:LANES, :] = jnp.where(marks > 0, -marks, (slots_t >> 9).astype(F32)).astype(BF16)
    table[LANES:, :] = jnp.where(marks > 0, 0.0, ((slots_t & 511) - 256).astype(F32)).astype(BF16)
    count_s[...] = jnp.zeros_like(count_s)

    def look_up(t, carry):
        block = keys_ref[pl.ds(t * tiles, tiles), :]
        key = jnp.concatenate([jnp.broadcast_to(block[i : i + 1, :], (8, LANES)) for i in range(tiles)], axis=1)
        found = mm(table[...], hot(1024, packed(key >> 7)))
        high = picked(found[:LANES], key & 127).astype(I32)
        low = picked(found[LANES:], key & 127).astype(I32)
        heavy = high < 0
        slot = jnp.where(heavy, -1 - (2 * (key >> 9) - 1 - high), high * 512 + low + 256)
        slot_s[:, pl.ds(t * step, step)] = slot
        major = jnp.where(heavy, -1, (slot >> 7) & 511)
        minor = ((slot >> 16) & 1) * LANES + (slot & 127)
        count_s[...] += mm_nt(hot(512, packed(major)), hot(256, packed(minor)))
        return carry

    lax.fori_loop(0, steps, look_up, 0, unroll=8)

    present = flag(count_s[...] > 0)
    a, b = iota((256, 512), 0), iota((256, 512), 1)
    b_in = b & 255
    same_half = (a >> 7) == (b_in >> 7)
    both = mm(present, flag(same_half & ((b >= 256) | (a < b_in))))
    a, b = iota((512, 512), 0), iota((512, 512), 1)
    earlier = flag((b < a) & ((a >> 4) == (b >> 4)))
    rank = both[:, :256] + mm(earlier, both[:, 256:].astype(BF16))
    table[0:LANES, 0:512] = rank[:, :LANES].T.astype(BF16)
    table[0:LANES, 512:1024] = rank[:, LANES:].T.astype(BF16)
    meta_s[...] = jnp.zeros_like(meta_s)

    def place(t, carry):
        slot = slot_s[:, pl.ds(t * step, step)]
        light = slot >= 0
        found = mm(table[0:LANES, :], hot(1024, packed(slot >> 7)))
        rank_here = picked(found, slot & 127).astype(I32)
        owner = slot >> 11
        peer = peer_of(owner)
        heavy_id = -1 - slot
        heavy_peer = peer_of(heavy_id >> 3) & 60 | (heavy_id >> 1) & 3
        heavy_id = heavy_peer * 8 + ((heavy_id >> 5) & 3) * 2 + (heavy_id & 1)
        at = jnp.where(light, (peer & 31) * 64 + rank_here, 2048 + (heavy_id & 255))
        place_s[:, pl.ds(t * step, step)] = packed(at)
        half = jnp.where(light, peer >> 5, heavy_id >> 8).astype(F32)
        rows_of = jnp.zeros((tiles, LANES), F32)
        for i in range(tiles):
            rows_of = jnp.where(iota((tiles, LANES), 0) == i, half[:, i * LANES : (i + 1) * LANES], rows_of)
        half_s[pl.ds(t * tiles, tiles), :] = rows_of
        owners = hot(64, packed(jnp.where(light, peer, -1)))
        inside = slot & 2047
        high = jnp.broadcast_to((inside >> 6).astype(F32)[0:1], (64, step)).astype(BF16)
        low = jnp.broadcast_to((inside & 63).astype(F32)[0:1], (64, step)).astype(BF16)
        left = jnp.concatenate(
            [owners, owners * high, owners * low, hot(16, packed(jnp.where(light, -1, heavy_id >> 5)))], axis=0
        )
        right = hot(LANES, packed(jnp.where(light, rank_here, 64 + (heavy_id & 31))))
        meta_s[...] += mm_nt(left, right)
        return carry

    lax.fori_loop(0, steps, place, 0, unroll=8)

    copy.wait()
    top = jnp.zeros((16, LANES), BF16)
    for i in range(row_count // 1024):
        piece = jnp.abs(rows[i * 1024 : (i + 1) * 1024, :]).reshape(64, 16, LANES)
        top = jnp.maximum(top, jnp.max(piece, axis=0))
    power = exponent(jnp.max(jnp.max(top.astype(F32), axis=0, keepdims=True), axis=1, keepdims=True))
    shrink_light = jnp.exp2(-8.0 - power)
    shrink_heavy = jnp.exp2(-13.0 - power)
    lane = iota((64, LANES), 1)
    number = meta_s[0:64, :]
    inside = jnp.where(
        number > 0,
        jnp.round(meta_s[64:128, :] / jnp.maximum(number, 1.0)) * 64.0
        + jnp.round(meta_s[128:192, :] / jnp.maximum(number, 1.0)),
        -1.0,
    )
    first = jnp.where(lane < 64, inside, pltpu.roll(number, 64, 1))
    groups = meta_s[192:208, :]
    spread = jnp.concatenate([jnp.broadcast_to(groups[i : i + 1, :], (4, LANES)) for i in range(16)], axis=0)
    owner_row = iota((64, LANES), 0)
    moved = jnp.zeros((64, LANES), F32)
    for c in range(4):
        moved = jnp.where((owner_row & 3) == c, pltpu.roll(spread, 64 - 8 * c, 1), moved)
    moved_high = jnp.floor(moved * (1.0 / 128.0))
    moved_low = moved - 128.0 * moved_high
    second = jnp.where(lane < 8, moved_low, jnp.where(lane < 16, pltpu.roll(moved_high, 8, 1), power))

    half_t = half_s[...].T
    for i in range(row_count // LANES):
        mine = jnp.broadcast_to(half_t[:, i : i + 1], (LANES, LANES)).astype(BF16)
        piece = rows[i * LANES : (i + 1) * LANES, :]
        second_half = piece * mine
        masked[i * LANES : (i + 1) * LANES, 0:LANES] = piece - second_half
        masked[i * LANES : (i + 1) * LANES, LANES:] = second_half

    def block_sums(b, count):
        total = jnp.zeros((count, 256), F32)
        for c in range(row_count // 1024):
            index = place_s[:, c * 1024 : (c + 1) * 1024] - (b * count).astype(I16)
            total += mm(hot(count, index), masked[c * 1024 : (c + 1) * 1024, :])
        return total

    def light_block(b, carry):
        total = coded(block_sums(b, 512), shrink_light)
        for h in range(2):
            piece = total[:, h * LANES : (h + 1) * LANES].astype(I32).astype(I16).reshape(8, 64, LANES)
            out_ref[pl.ds(h * 32 + b * 8, 8), 0:64, :] = piece
        return carry

    lax.fori_loop(0, 4, light_block, 0, unroll=2)
    total = coded(block_sums(jnp.int32(8), 256), shrink_heavy)
    turned = jnp.concatenate([total[:, :LANES].T, total[:, LANES:].T], axis=1)
    sums = jnp.concatenate([turned[:, k * LANES : (k + 1) * LANES].reshape(64, 2, LANES) for k in range(4)], axis=1)
    sub = iota((64, 8, LANES), 1)
    extra = jnp.where(sub == 0, first[:, None, :], jnp.where(sub == 1, second[:, None, :], 0.0))
    out_ref[:, 64:80, :] = jnp.concatenate([sums, extra], axis=1).astype(I32).astype(I16)


def pack(row_keys, key_slot, heavy_keys, measures):
    n = measures.shape[0]
    return pl.pallas_call(
        pack_kernel,
        out_shape=pltpu.VMEM((64, 80, LANES), I16),
        in_specs=[pl.BlockSpec(memory_space=pltpu.VMEM)] * 3 + [pl.BlockSpec(memory_space=pl.ANY)],
        scratch_shapes=[
            pltpu.VMEM((n, LANES), BF16),
            pltpu.VMEM((256, 1024), BF16),
            pltpu.VMEM((8, n), I32),
            pltpu.VMEM((16, n), I16),
            pltpu.VMEM((n // LANES, LANES), F32),
            pltpu.VMEM((512, 256), F32),
            pltpu.VMEM((208, LANES), F32),
            pltpu.VMEM((n, 256), BF16),
            pltpu.SemaphoreType.DMA,
        ],
        compiler_params=pltpu.CompilerParams(vmem_limit_bytes=56 * 2**20),
        name="pack",
    )(row_keys.reshape(-1, LANES), key_slot.reshape(-1, LANES), heavy_keys.reshape(-1, LANES), measures)


def label_kernel(me_ref, slots_ref, out_ref):
    slots = slots_ref[...]
    mine = (slots >> 11) == me_ref[0]
    inside = (slots & 2047).astype(F32)
    a, b = iota((LANES, 256), 0), iota((LANES, 256), 1)
    both = mm(flag(mine), flag((b >= LANES) | (a < b)))
    a, b = iota((256, 256), 0), iota((256, 256), 1)
    earlier = flag((b < a) & ((a >> 2) == (b >> 2)))
    lane = iota((256, LANES), 1)
    rows = []
    for c in range(4):
        part = slice(c * 256, (c + 1) * 256)
        rank = both[part, :LANES] + mm(earlier, both[part, LANES:].astype(BF16))
        found = jnp.zeros((256, LANES), F32)
        for j in range(8):
            value = jnp.where(mine[part] & (rank == float(j)), inside[part], 0.0)
            found = jnp.where(lane == j, jnp.sum(value, axis=1, keepdims=True), found)
        rows.append(jnp.sum(found.reshape(64, 4, LANES), axis=1))
    out_ref[...] = jnp.concatenate(rows, axis=0)


def labels_of(owner, key_slot):
    order = key_slot.reshape(4, 4, 16, 4, LANES).transpose(1, 0, 2, 3, 4).reshape(1024, LANES)
    return pl.pallas_call(
        label_kernel,
        out_shape=pltpu.VMEM((256, LANES), F32),
        in_specs=[pl.BlockSpec(memory_space=pltpu.SMEM), pl.BlockSpec(memory_space=pltpu.VMEM)],
        name="labels",
    )(owner.reshape(1), order)


def slot_sums(labels, index_s, pair_s):
    column = jnp.concatenate([jnp.broadcast_to(labels[:, j : j + 1], (64, LANES)) for j in range(8)], axis=0)
    column = column.astype(I32).astype(I16).reshape(32, 16, LANES)
    total = jnp.zeros((512, 256), F32)
    for c in range(0, 4096, 1024):
        hots = jnp.concatenate(
            [
                jnp.where(column == index_s[:, c + i : c + i + LANES][None], BF16(1), BF16(0)).reshape(512, LANES)
                for i in range(0, 1024, LANES)
            ],
            axis=1,
        )
        total += mm(hots, pair_s[c : c + 1024, :])
    return total[:, :LANES] + total[:, LANES:]


def owner_kernel(me_ref, got_ref, label_ref, out_ref, r0_ref, r1_ref, r2_ref, r3_ref, pair_s, index_s, weight_s):
    sources = got_ref.shape[0]
    tail = got_ref[:, 64:80, :].astype(F32)
    first = tail[:, 8, :]
    second = tail[:, 9, :]
    stretch = jnp.exp2(tail[:, 9:10, LANES - 1 :] + 8.0)
    heavy = jnp.sum(decoded(tail[:, 0:8, :], stretch * 32.0), axis=0)
    heavy_counts = jnp.sum(second, axis=0, keepdims=True)

    swapped = pltpu.roll(first, 64, 1)
    low_lane = iota((1, LANES), 1) < 64
    for i in range(sources // 2):
        even, odd = slice(2 * i, 2 * i + 1), slice(2 * i + 1, 2 * i + 2)
        at = slice(i * LANES, (i + 1) * LANES)
        index = jnp.where(low_lane, first[even], swapped[odd]).astype(I32)
        index_s[:, at] = packed(jnp.broadcast_to(index, (8, LANES)))
        weight = jnp.where(low_lane, swapped[even], first[odd])
        weight_s[:, at] = jnp.broadcast_to(weight, (16, LANES)).astype(BF16)

    for s in range(0, sources, 8):
        values = decoded(got_ref[s : s + 8, 0:64, :].astype(I32), stretch[s : s + 8]).reshape(512, LANES)
        high, low = split2(values)
        pair_s[s * 64 : (s + 8) * 64, 0:LANES] = high
        pair_s[s * 64 : (s + 8) * 64, LANES:] = low

    wide = index_s[...].astype(I32)[0:8]
    histogram = mm_nt(hot(16, packed(wide >> 7)) * weight_s[...], hot(LANES, packed(wide & 127)))

    for i, rows_ref in enumerate((r0_ref, r1_ref, r2_ref, r3_ref)):
        q = (me_ref[0] + i) & 3
        rows = histogram[0:4]
        for p in range(1, 4):
            rows = jnp.where(q == p, histogram[4 * p : 4 * p + 4], rows)
        rows_ref[...] = rows

    heavy_top = jnp.max(jnp.max(jnp.abs(heavy), axis=0, keepdims=True), axis=1, keepdims=True)
    heavy_power = exponent(heavy_top)
    heavy_code = coded(heavy, jnp.exp2(-heavy_power))
    member = iota((64, LANES), 0)
    heavy_lines = []
    for c in range(2):
        line = jnp.broadcast_to(heavy_code[c : c + 1], (64, LANES))
        for k in range(1, 4):
            line = jnp.where((member >> 4) == k, heavy_code[2 * k + c : 2 * k + c + 1], line)
        heavy_lines.append(line)
    one_lane = iota((1, LANES), 1)

    lane = iota((64, LANES), 1)
    quarter = iota((64, LANES), 0) & 3
    lines = []
    for i in range(4):
        line = jnp.broadcast_to(histogram[i : i + 1], (64, LANES))
        for q in range(1, 4):
            line = jnp.where(quarter == q, histogram[4 * q + i : 4 * q + i + 1], line)
        lines.append(line)
    for t in range(4):
        labels = label_ref[t * 64 : (t + 1) * 64, :]
        total = slot_sums(labels, index_s, pair_s)
        top = jnp.max(jnp.abs(total), axis=0, keepdims=True)
        power = exponent(jnp.max(top, axis=1, keepdims=True))
        code = coded(total, jnp.exp2(-power)).astype(I32)
        for j in range(4):
            word = (code[j * 64 : (j + 1) * 64] << 16) | (code[(j + 4) * 64 : (j + 5) * 64] & 65535)
            out_ref[pl.ds(t * 320 + j, 64, stride=5), :] = word
        inside = labels.astype(I32) & 511
        found = jnp.broadcast_to(power, (64, LANES))
        for j in range(8):
            column = jnp.broadcast_to(inside[:, j : j + 1], (64, LANES))
            number = jnp.zeros((64, LANES), F32)
            for i in range(4):
                number += jnp.where(column == lane + i * LANES, lines[i], 0.0)
            found = jnp.where(lane == j, jnp.sum(number, axis=1, keepdims=True), found)
        found = jnp.where(lane == 126, heavy_power, found).astype(I32)
        for h in range(2):
            spot = t * 2 + h
            hit = lane == (member & 15) * 8 + spot
            code = [jnp.sum(jnp.where(hit, line, 0.0), axis=1, keepdims=True).astype(I32) for line in heavy_lines]
            count = jnp.where(one_lane == spot, heavy_counts, 0.0) + jnp.where(one_lane == spot + 8, heavy_counts * 128.0, 0.0)
            count = jnp.sum(count, axis=1, keepdims=True).astype(I32)
            found = jnp.where(lane == 8 + h, (code[0] << 16) | (code[1] & 65535), jnp.where(lane == 10 + h, count, found))
        out_ref[pl.ds(t * 320 + 4, 64, stride=5), :] = found


def owner_sums(index_t, got, labels):
    vmem = pl.BlockSpec(memory_space=pltpu.VMEM)
    return pl.pallas_call(
        owner_kernel,
        out_shape=(pltpu.VMEM((1280, LANES), I32),) + (jax.ShapeDtypeStruct((4, LANES), F32),) * 4,
        in_specs=[pl.BlockSpec(memory_space=pltpu.SMEM), vmem, vmem],
        scratch_shapes=[pltpu.VMEM((4096, 256), BF16), pltpu.VMEM((16, 4096), I16), pltpu.VMEM((16, 4096), BF16)],
        compiler_params=pltpu.CompilerParams(vmem_limit_bytes=32 * 2**20),
        name="owner",
    )(index_t.reshape(1), near(got), near(labels))


def place_kernel(slots_ref, out_ref):
    owner = peer_of(slots_ref[...] >> 11)
    wide = jnp.concatenate([jnp.broadcast_to(owner[i : i + 1, :], (8, LANES)) for i in range(4)], axis=1)
    padded = jnp.concatenate([owner, owner], axis=0)
    turned = padded.astype(F32).T.astype(I32)
    earlier = jnp.zeros((8, 512), F32)
    k = iota((16, 8, 512), 2)
    for i in range(4):
        column = jnp.broadcast_to(turned[:, i : i + 1], (LANES, 512)).reshape(16, 8, 512)
        other = iota((LANES, 512), 0).reshape(16, 8, 512) + i * LANES
        earlier += jnp.sum(jnp.where((column == wide[None]) & (other < k), 1.0, 0.0), axis=0)
    place = wide.astype(F32) + 64.0 * jnp.sum(earlier, axis=0, keepdims=True)
    rows = jnp.concatenate([place[0:1, i * LANES : (i + 1) * LANES] for i in range(4)] * 2, axis=0)
    columns = rows.T
    for i in range(4):
        spot = jnp.broadcast_to(columns[:, i : i + 1], (LANES, 512)).astype(I32)
        out_ref[i * LANES : (i + 1) * LANES, :] = flag(spot == iota((LANES, 512), 1))


def places(slots_here):
    return pl.pallas_call(place_kernel, out_shape=pltpu.VMEM((512, 512), BF16), name="places")(slots_here)


def join_kernel(heavy_ref, me_ref, got_ref, place_ref, orders_ref, out_ref, report_ref, joined_s):
    lines = [got_ref[pl.ds(t * 320 + 4, 64, stride=5), :] for t in range(4)]
    stretch = [jnp.exp2(line[:, LANES - 1 :].astype(F32)) for line in lines]
    found = (lines[0] + lines[1] + lines[2] + lines[3]).astype(F32)
    lane, member = iota((64, LANES), 1), iota((64, LANES), 0)
    heavy_sums, heavy_counts = [], []
    for h in range(2):
        row = jnp.zeros((64, LANES), F32)
        count = jnp.zeros((64, LANES), F32)
        for line in lines:
            word = line[:, 8 + h : 9 + h]
            scale = jnp.exp2(line[:, 126:127].astype(F32))
            row += jnp.where(lane == 2 * member, decoded(word >> 16, scale), 0.0)
            row += jnp.where(lane == 2 * member + 1, decoded((word << 16) >> 16, scale), 0.0)
            count += jnp.where((member == me_ref[0]) & (lane == 10 + h), line, 0).astype(F32)
        heavy_sums.append(jnp.sum(row, axis=0, keepdims=True))
        heavy_counts.append(jnp.sum(jnp.sum(count, axis=0, keepdims=True), axis=1, keepdims=True))
    above, below = [], []
    for j in range(4):
        words = [got_ref[pl.ds(t * 320 + j, 64, stride=5), :] for t in range(4)]
        above.append(sum(decoded(word >> 16, s) for word, s in zip(words, stretch)))
        below.append(sum(decoded((word << 16) >> 16, s) for word, s in zip(words, stretch)))
    sums = jnp.concatenate(above + below, axis=0)
    high = jnp.floor(found * (1.0 / 128.0)) * 128.0
    low = found - high
    low = jnp.concatenate([jnp.broadcast_to(low[:, j : j + 1], (64, LANES)) for j in range(8)], axis=0).astype(BF16)
    high = jnp.concatenate([jnp.broadcast_to(high[:, j : j + 1], (64, LANES)) for j in range(8)], axis=0)
    high_a, high_b = split2(high)
    sum_a, sum_b = split2(sums)
    right = jnp.concatenate([sum_a, sum_b, low, high_a, high_b], axis=1)

    for i in range(4):
        part = slice(i * LANES, (i + 1) * LANES)
        moved = mm(place_ref[part, :], right)
        total = moved[:, 0:LANES] + moved[:, LANES : 2 * LANES]
        number = moved[:, 2 * LANES : 3 * LANES] + (moved[:, 3 * LANES : 4 * LANES] + moved[:, 4 * LANES :])
        key = iota((LANES, LANES), 0) + i * LANES
        for h in range(2):
            hit = key == heavy_ref[h]
            total = jnp.where(hit, heavy_sums[h], total)
            number = jnp.where(hit, heavy_counts[h], number)
        joined = orders_ref[part, :].astype(F32) * total * lax.rsqrt(1.0 + number)
        joined_s[part, :] = joined
        out_ref[part, :] = joined.astype(BF16)
    report_ref[...] = jnp.concatenate(
        [joined_s[pl.ds(heavy_ref[0], 1), :], joined_s[pl.ds(heavy_ref[1], 1), :]], axis=0
    ).astype(BF16)


def join(heavy_here, member, got, place, orders):
    vmem = pl.BlockSpec(memory_space=pltpu.VMEM)
    smem = pl.BlockSpec(memory_space=pltpu.SMEM)
    return pl.pallas_call(
        join_kernel,
        out_shape=(jax.ShapeDtypeStruct((512, LANES), BF16), jax.ShapeDtypeStruct((2, LANES), BF16)),
        in_specs=[smem, smem, vmem, vmem, vmem],
        scratch_shapes=[pltpu.VMEM((512, LANES), F32)],
        name="join",
    )(heavy_here, member.reshape(1), near(got), near(place), orders)


def swap(x):
    return lax.all_to_all(x, GROUP, split_axis=0, concat_axis=0, tiled=True)


def body(measures, row_keys, orders, heavy_keys, key_slot):
    x, t, low, core, y = (lax.axis_index(name) for name in AXES)
    device = (((x * 4 + t) * 2 + low) * 2 + core) * 4 + y
    owner = ((x * 4 + y) * 2 + low) * 2 + core
    got = swap(pack(row_keys, key_slot, heavy_keys, measures))
    labels = labels_of(owner, key_slot)
    words, *rows = owner_sums(t, got, labels)
    got = lax.all_to_all(words.reshape(256, 1, 640), ("t",) + GROUP, split_axis=0, concat_axis=0, tiled=True)
    got = got.reshape(1280, LANES)
    slot_rows = sum(
        lax.ppermute(rows[i], ("t", "y"), [(4 * a + b, 4 * b + (a + i) % 4) for a in range(4) for b in range(4)])
        for i in range(4)
    )
    heavy_here = lax.dynamic_slice_in_dim(heavy_keys, device * 2, 2) - device * 512
    slots_here = lax.dynamic_slice_in_dim(key_slot, device * 512, 512).reshape(4, LANES)
    result, report = join(heavy_here, ((x * 2 + low) * 2 + core) * 4 + y, got, places(slots_here), orders)
    return result, report, slot_rows.reshape(512)


def solution(mesh):
    split = Mesh(mesh.devices.reshape(4, 4, 2, 2, 4), AXES)
    return jax.shard_map(
        body,
        mesh=split,
        in_specs=(P(AXES, None), P(AXES), P(AXES, None), P(), P()),
        out_specs=(P(AXES, None), P(AXES, None), P(AXES)),
        check_vma=False,
    )
```

```python
import jax
import jax.numpy as jnp
from jax import lax
from jax.experimental import pallas as pl
from jax.experimental.pallas import tpu as pltpu
from jax.sharding import Mesh
from jax.sharding import PartitionSpec as P

F32, BF16, I16, I32 = jnp.float32, jnp.bfloat16, jnp.int16, jnp.int32
LANES = 128
CODE = 32767.0
TINY = 1e-37
AXES = ("x", "t", "low", "core", "y")
GROUP = ("x", "low", "core", "y")


def near(x):
    return pltpu.with_memory_space_constraint(x, pltpu.VMEM)


def iota(shape, dim, dtype=I32):
    return lax.broadcasted_iota(dtype, shape, dim)


def packed(index):
    return jnp.concatenate([index, index], axis=0).astype(I16)


def hot(count, index):
    n = index.shape[1]
    label = iota((count, n), 0, I16).reshape(count // 16, 16, n)
    return jnp.where(label == index[None], BF16(1), BF16(0)).reshape(count, n)


def mm(a, b):
    return lax.dot_general(a, b, (((1,), (0,)), ((), ())), preferred_element_type=F32)


def mm_nt(a, b):
    return lax.dot_general(a, b, (((1,), (1,)), ((), ())), preferred_element_type=F32)


def flag(mask):
    return jnp.where(mask, 1.0, 0.0).astype(BF16)


def picked(table, index):
    n = index.shape[1]
    hit = iota((LANES, n), 0).reshape(LANES // 8, 8, n) == index[None]
    part = jnp.sum(jnp.where(hit, table.reshape(LANES // 8, 8, n), 0.0), axis=0)
    return jnp.broadcast_to(jnp.sum(part, axis=0, keepdims=True), (8, n))


def exponent(top):
    return jnp.ceil(jnp.log2(jnp.maximum(top, TINY))) + 1.0


def coded(x, shrink):
    y = jnp.sqrt(jnp.sqrt(jnp.abs(x) * shrink)) * CODE + 0.5
    return jnp.where(x < 0, -y, y)


def decoded(code, stretch):
    t = code.astype(F32) * (1.0 / CODE)
    s = t * t
    return s * s * jnp.where(t < 0, -stretch, stretch)


def two(a, b):
    return (a << 16) | (b & 65535)


def split2(x):
    high = x.astype(BF16)
    return high, (x - high.astype(F32)).astype(BF16)


def peer_of(owner):
    return (owner & 48) | ((owner & 3) << 2) | ((owner >> 2) & 3)


def pack_kernel(
    keys_ref, slots_ref, heavy_ref, rows_hbm, out_ref, rows, table, slot_s, place_s, half_s, count_s, meta_s, masked, sem, word_s
):
    row_count = rows.shape[0]
    step = 1024
    tiles = step // LANES
    steps = row_count // step
    copy = pltpu.make_async_copy(rows_hbm, rows, sem)
    copy.start()

    slots_t = slots_ref[...].T
    hk = jnp.concatenate([heavy_ref[i : i + 1, :] for i in range(4)], axis=1)
    hk = jnp.broadcast_to(hk, (8, 512))
    weight = (1 + (iota((LANES, 512), 1) & 1)).astype(BF16)
    marks = mm_nt(hot(LANES, packed(hk & 127)) * weight, hot(1024, packed(hk >> 7)))
    table[0:LANES, :] = jnp.where(marks > 0, -marks, (slots_t >> 9).astype(F32)).astype(BF16)
    table[LANES:, :] = jnp.where(marks > 0, 0.0, ((slots_t & 511) - 256).astype(F32)).astype(BF16)
    count_s[...] = jnp.zeros_like(count_s)

    def look_up(t, carry):
        block = keys_ref[pl.ds(t * tiles, tiles), :]
        key = jnp.concatenate([jnp.broadcast_to(block[i : i + 1, :], (8, LANES)) for i in range(tiles)], axis=1)
        found = mm(table[...], hot(1024, packed(key >> 7)))
        high = picked(found[:LANES], key & 127).astype(I32)
        low = picked(found[LANES:], key & 127).astype(I32)
        heavy = high < 0
        slot = jnp.where(heavy, -1 - (2 * (key >> 9) - 1 - high), high * 512 + low + 256)
        slot_s[:, pl.ds(t * step, step)] = slot
        major = jnp.where(heavy, -1, (slot >> 7) & 511)
        minor = ((slot >> 16) & 1) * LANES + (slot & 127)
        count_s[...] += mm_nt(hot(512, packed(major)).astype(jnp.float8_e4m3fn), hot(256, packed(minor)).astype(jnp.float8_e4m3fn))
        return carry

    lax.fori_loop(0, steps, look_up, 0, unroll=8)

    present = flag(count_s[...] > 0)
    a, b = iota((256, 512), 0), iota((256, 512), 1)
    b_in = b & 255
    same_half = (a >> 7) == (b_in >> 7)
    both = mm(present, flag(same_half & ((b >= 256) | (a < b_in))))
    a, b = iota((512, 512), 0), iota((512, 512), 1)
    earlier = flag((b < a) & ((a >> 4) == (b >> 4)))
    rank = both[:, :256] + mm(earlier, both[:, 256:].astype(BF16))
    table[0:LANES, 0:512] = rank[:, :LANES].T.astype(BF16)
    table[0:LANES, 512:1024] = rank[:, LANES:].T.astype(BF16)
    meta_s[...] = jnp.zeros_like(meta_s)

    def place(t, carry):
        slot = slot_s[:, pl.ds(t * step, step)]
        light = slot >= 0
        found = mm(table[0:LANES, :], hot(1024, packed(slot >> 7)))
        rank_here = picked(found, slot & 127).astype(I32)
        owner = slot >> 11
        peer = peer_of(owner)
        heavy_id = -1 - slot
        heavy_peer = peer_of(heavy_id >> 3) & 60 | (heavy_id >> 1) & 3
        heavy_id = heavy_peer * 8 + ((heavy_id >> 5) & 3) * 2 + (heavy_id & 1)
        at = jnp.where(light, (peer & 31) * 64 + rank_here, 2048 + (heavy_id & 255))
        place_s[:, pl.ds(t * step, step)] = packed(at)
        half = jnp.where(light, peer >> 5, heavy_id >> 8).astype(F32)
        rows_of = jnp.zeros((tiles, LANES), F32)
        for i in range(tiles):
            rows_of = jnp.where(iota((tiles, LANES), 0) == i, half[:, i * LANES : (i + 1) * LANES], rows_of)
        half_s[pl.ds(t * tiles, tiles), :] = rows_of
        owners = hot(64, packed(jnp.where(light, peer, -1)))
        inside = slot & 2047
        high = jnp.broadcast_to((inside >> 6).astype(F32)[0:1], (64, step)).astype(BF16)
        low = jnp.broadcast_to((inside & 63).astype(F32)[0:1], (64, step)).astype(BF16)
        left = jnp.concatenate(
            [owners, owners * high, owners * low, hot(16, packed(jnp.where(light, -1, heavy_id >> 5)))], axis=0
        )
        right = hot(LANES, packed(jnp.where(light, rank_here, 64 + (heavy_id & 31))))
        meta_s[...] += mm_nt(left, right)
        return carry

    lax.fori_loop(0, steps, place, 0, unroll=8)

    copy.wait()
    top = jnp.zeros((16, LANES), BF16)
    for i in range(row_count // 1024):
        piece = jnp.abs(rows[i * 1024 : (i + 1) * 1024, :]).reshape(64, 16, LANES)
        top = jnp.maximum(top, jnp.max(piece, axis=0))
    power = exponent(jnp.max(jnp.max(top.astype(F32), axis=0, keepdims=True), axis=1, keepdims=True))
    shrink_light = jnp.exp2(-8.0 - power)
    shrink_heavy = jnp.exp2(-13.0 - power)
    lane = iota((64, LANES), 1)
    number = meta_s[0:64, :]
    inside = jnp.where(
        number > 0,
        jnp.round(meta_s[64:128, :] / jnp.maximum(number, 1.0)) * 64.0
        + jnp.round(meta_s[128:192, :] / jnp.maximum(number, 1.0)),
        -1.0,
    )
    first = jnp.where(lane < 64, inside, pltpu.roll(number, 64, 1))
    groups = meta_s[192:208, :]
    spread = jnp.concatenate([jnp.broadcast_to(groups[i : i + 1, :], (4, LANES)) for i in range(16)], axis=0)
    owner_row = iota((64, LANES), 0)
    moved = jnp.zeros((64, LANES), F32)
    for c in range(4):
        moved = jnp.where((owner_row & 3) == c, pltpu.roll(spread, 64 - 8 * c, 1), moved)
    moved_high = jnp.floor(moved * (1.0 / 128.0))
    moved_low = moved - 128.0 * moved_high
    second = jnp.where(lane < 8, moved_low, jnp.where(lane < 16, pltpu.roll(moved_high, 8, 1), power))

    half_t = half_s[...].T
    for i in range(row_count // LANES):
        mine = jnp.broadcast_to(half_t[:, i : i + 1], (LANES, LANES)).astype(BF16)
        piece = rows[i * LANES : (i + 1) * LANES, :]
        second_half = piece * mine
        masked[i * LANES : (i + 1) * LANES, 0:LANES] = piece - second_half
        masked[i * LANES : (i + 1) * LANES, LANES:] = second_half

    def block_sums(b, count):
        total = jnp.zeros((count, 256), F32)
        for c in range(row_count // 1024):
            index = place_s[:, c * 1024 : (c + 1) * 1024] - (b * count).astype(I16)
            total += mm(hot(count, index), masked[c * 1024 : (c + 1) * 1024, :])
        return total

    def light_block(b, carry):
        total = coded(block_sums(b, 512), shrink_light)
        for h in range(2):
            piece = total[:, h * LANES : (h + 1) * LANES].astype(I32).reshape(8, 64, LANES)
            words = two(piece[:, :32], piece[:, 32:])
            for i in range(8):
                out_ref[pl.ds((h * 32 + b * 8 + i) * 37, 32), :] = words[i]
        return carry

    lax.fori_loop(0, 4, light_block, 0, unroll=2)
    total = coded(block_sums(jnp.int32(8), 256), shrink_heavy)
    turned = jnp.concatenate([total[:, :LANES].T, total[:, LANES:].T], axis=1).astype(I32)
    for k in range(2):
        word_s[...] = two(turned[:, k * LANES : (k + 1) * LANES], turned[:, (k + 2) * LANES : (k + 3) * LANES])
        for c in range(2):
            out_ref[pl.ds(32 + 2 * k + c, 64, stride=37), :] = word_s[pl.ds(c, 64, stride=2), :]
    words = two(first.astype(I32), pltpu.roll(first, 64, 1).astype(I32))
    out_ref[pl.ds(36, 64, stride=37), :] = jnp.where(lane < 64, words, pltpu.roll(second, 64, 1).astype(I32))


def pack(row_keys, key_slot, heavy_keys, measures):
    n = measures.shape[0]
    return pl.pallas_call(
        pack_kernel,
        out_shape=pltpu.VMEM((2368, LANES), I32),
        in_specs=[pl.BlockSpec(memory_space=pltpu.VMEM)] * 3 + [pl.BlockSpec(memory_space=pl.ANY)],
        scratch_shapes=[
            pltpu.VMEM((n, LANES), BF16),
            pltpu.VMEM((256, 1024), BF16),
            pltpu.VMEM((8, n), I32),
            pltpu.VMEM((16, n), I16),
            pltpu.VMEM((n // LANES, LANES), F32),
            pltpu.VMEM((512, 256), F32),
            pltpu.VMEM((208, LANES), F32),
            pltpu.VMEM((n, 256), BF16),
            pltpu.SemaphoreType.DMA,
            pltpu.VMEM((LANES, LANES), I32),
        ],
        compiler_params=pltpu.CompilerParams(vmem_limit_bytes=56 * 2**20),
        name="pack",
    )(row_keys.reshape(-1, LANES), key_slot.reshape(-1, LANES), heavy_keys.reshape(-1, LANES), measures)


def label_kernel(me_ref, slots_ref, out_ref):
    slots = slots_ref[...]
    mine = (slots >> 11) == me_ref[0]
    inside = (slots & 2047).astype(F32)
    a, b = iota((LANES, 256), 0), iota((LANES, 256), 1)
    both = mm(flag(mine), flag((b >= LANES) | (a < b)))
    a, b = iota((256, 256), 0), iota((256, 256), 1)
    earlier = flag((b < a) & ((a >> 2) == (b >> 2)))
    lane = iota((256, LANES), 1)
    rows = []
    for c in range(4):
        part = slice(c * 256, (c + 1) * 256)
        rank = both[part, :LANES] + mm(earlier, both[part, LANES:].astype(BF16))
        found = jnp.zeros((256, LANES), F32)
        for j in range(8):
            value = jnp.where(mine[part] & (rank == float(j)), inside[part], 0.0)
            found = jnp.where(lane == j, jnp.sum(value, axis=1, keepdims=True), found)
        rows.append(jnp.sum(found.reshape(64, 4, LANES), axis=1))
    out_ref[...] = jnp.concatenate(rows, axis=0)


def labels_of(owner, key_slot):
    order = key_slot.reshape(4, 4, 16, 4, LANES).transpose(1, 0, 2, 3, 4).reshape(1024, LANES)
    return pl.pallas_call(
        label_kernel,
        out_shape=pltpu.VMEM((256, LANES), F32),
        in_specs=[pl.BlockSpec(memory_space=pltpu.SMEM), pl.BlockSpec(memory_space=pltpu.VMEM)],
        name="labels",
    )(owner.reshape(1), order)


def slot_sums(labels, index_s, pair_s):
    column = jnp.concatenate([jnp.broadcast_to(labels[:, j : j + 1], (64, LANES)) for j in range(8)], axis=0)
    column = column.astype(I32).astype(I16).reshape(32, 16, LANES)
    total = jnp.zeros((512, 256), F32)
    for c in range(0, 4096, 1024):
        hots = jnp.concatenate(
            [
                jnp.where(column == index_s[:, c + i : c + i + LANES][None], BF16(1), BF16(0)).reshape(512, LANES)
                for i in range(0, 1024, LANES)
            ],
            axis=1,
        )
        total += mm(hots, pair_s[c : c + 1024, :])
    return total[:, :LANES] + total[:, LANES:]


def owner_kernel(me_ref, got_ref, label_ref, out_ref, r0_ref, r1_ref, r2_ref, r3_ref, pair_s, index_s, weight_s):
    sources = 64
    meta = got_ref[pl.ds(36, 64, stride=37), :]
    second = pltpu.roll(meta, 64, 1).astype(F32)
    counts = (meta & 65535).astype(F32)
    first = jnp.where(iota((64, LANES), 1) < 64, (meta >> 16).astype(F32), pltpu.roll(counts, 64, 1))
    stretch = jnp.exp2(meta[:, LANES - 1 :].astype(F32) + 8.0)
    heavy = [got_ref[pl.ds(32 + r, 64, stride=37), :] for r in range(4)]
    heavy = [decoded(word >> 16, stretch * 32.0) for word in heavy] + [decoded((word << 16) >> 16, stretch * 32.0) for word in heavy]
    heavy = jnp.concatenate([jnp.sum(part, axis=0, keepdims=True) for part in heavy], axis=0)
    heavy_counts = jnp.sum(second, axis=0, keepdims=True)

    swapped = pltpu.roll(first, 64, 1)
    low_lane = iota((1, LANES), 1) < 64
    for i in range(sources // 2):
        even, odd = slice(2 * i, 2 * i + 1), slice(2 * i + 1, 2 * i + 2)
        at = slice(i * LANES, (i + 1) * LANES)
        index = jnp.where(low_lane, first[even], swapped[odd]).astype(I32)
        index_s[:, at] = packed(jnp.broadcast_to(index, (8, LANES)))
        weight = jnp.where(low_lane, swapped[even], first[odd])
        weight_s[:, at] = jnp.broadcast_to(weight, (16, LANES)).astype(BF16)

    for s in range(sources):
        word = got_ref[s * 37 : s * 37 + 32, :]
        scale = stretch[s : s + 1]
        for i, code in enumerate((word >> 16, (word << 16) >> 16)):
            high, low = split2(decoded(code, scale))
            at = slice(s * 64 + i * 32, s * 64 + i * 32 + 32)
            pair_s[at, 0:LANES] = high
            pair_s[at, LANES:] = low

    wide = index_s[...].astype(I32)[0:8]
    histogram = mm_nt(hot(16, packed(wide >> 7)) * weight_s[...], hot(LANES, packed(wide & 127)))

    for i, rows_ref in enumerate((r0_ref, r1_ref, r2_ref, r3_ref)):
        q = (me_ref[0] + i) & 3
        rows = histogram[0:4]
        for p in range(1, 4):
            rows = jnp.where(q == p, histogram[4 * p : 4 * p + 4], rows)
        rows_ref[...] = rows

    heavy_top = jnp.max(jnp.max(jnp.abs(heavy), axis=0, keepdims=True), axis=1, keepdims=True)
    heavy_power = exponent(heavy_top)
    heavy_code = coded(heavy, jnp.exp2(-heavy_power))
    member = iota((64, LANES), 0)
    heavy_lines = []
    for c in range(2):
        line = jnp.broadcast_to(heavy_code[c : c + 1], (64, LANES))
        for k in range(1, 4):
            line = jnp.where((member >> 4) == k, heavy_code[2 * k + c : 2 * k + c + 1], line)
        heavy_lines.append(line)
    one_lane = iota((1, LANES), 1)

    lane = iota((64, LANES), 1)
    quarter = iota((64, LANES), 0) & 3
    lines = []
    for i in range(4):
        line = jnp.broadcast_to(histogram[i : i + 1], (64, LANES))
        for q in range(1, 4):
            line = jnp.where(quarter == q, histogram[4 * q + i : 4 * q + i + 1], line)
        lines.append(line)
    for t in range(4):
        labels = label_ref[t * 64 : (t + 1) * 64, :]
        total = slot_sums(labels, index_s, pair_s)
        top = jnp.max(jnp.abs(total), axis=0, keepdims=True)
        power = exponent(jnp.max(top, axis=1, keepdims=True))
        code = coded(total, jnp.exp2(-power)).astype(I32)
        for j in range(4):
            word = (code[j * 64 : (j + 1) * 64] << 16) | (code[(j + 4) * 64 : (j + 5) * 64] & 65535)
            out_ref[pl.ds(t * 320 + j, 64, stride=5), :] = word
        inside = labels.astype(I32) & 511
        found = jnp.broadcast_to(power, (64, LANES))
        for j in range(8):
            column = jnp.broadcast_to(inside[:, j : j + 1], (64, LANES))
            number = jnp.zeros((64, LANES), F32)
            for i in range(4):
                number += jnp.where(column == lane + i * LANES, lines[i], 0.0)
            found = jnp.where(lane == j, jnp.sum(number, axis=1, keepdims=True), found)
        found = jnp.where(lane == 126, heavy_power, found).astype(I32)
        for h in range(2):
            spot = t * 2 + h
            hit = lane == (member & 15) * 8 + spot
            code = [jnp.sum(jnp.where(hit, line, 0.0), axis=1, keepdims=True).astype(I32) for line in heavy_lines]
            count = jnp.where(one_lane == spot, heavy_counts, 0.0) + jnp.where(one_lane == spot + 8, heavy_counts * 128.0, 0.0)
            count = jnp.sum(count, axis=1, keepdims=True).astype(I32)
            found = jnp.where(lane == 8 + h, (code[0] << 16) | (code[1] & 65535), jnp.where(lane == 10 + h, count, found))
        out_ref[pl.ds(t * 320 + 4, 64, stride=5), :] = found


def owner_sums(index_t, got, labels):
    vmem = pl.BlockSpec(memory_space=pltpu.VMEM)
    return pl.pallas_call(
        owner_kernel,
        out_shape=(pltpu.VMEM((1280, LANES), I32),) + (jax.ShapeDtypeStruct((4, LANES), F32),) * 4,
        in_specs=[pl.BlockSpec(memory_space=pltpu.SMEM), vmem, vmem],
        scratch_shapes=[pltpu.VMEM((4096, 256), BF16), pltpu.VMEM((16, 4096), I16), pltpu.VMEM((16, 4096), BF16)],
        compiler_params=pltpu.CompilerParams(vmem_limit_bytes=32 * 2**20),
        name="owner",
    )(index_t.reshape(1), near(got), near(labels))


def place_kernel(slots_ref, out_ref):
    owner = peer_of(slots_ref[...] >> 11)
    wide = jnp.concatenate([jnp.broadcast_to(owner[i : i + 1, :], (8, LANES)) for i in range(4)], axis=1)
    padded = jnp.concatenate([owner, owner], axis=0)
    turned = padded.astype(F32).T.astype(I32)
    earlier = jnp.zeros((8, 512), F32)
    k = iota((16, 8, 512), 2)
    for i in range(4):
        column = jnp.broadcast_to(turned[:, i : i + 1], (LANES, 512)).reshape(16, 8, 512)
        other = iota((LANES, 512), 0).reshape(16, 8, 512) + i * LANES
        earlier += jnp.sum(jnp.where((column == wide[None]) & (other < k), 1.0, 0.0), axis=0)
    place = wide.astype(F32) + 64.0 * jnp.sum(earlier, axis=0, keepdims=True)
    rows = jnp.concatenate([place[0:1, i * LANES : (i + 1) * LANES] for i in range(4)] * 2, axis=0)
    columns = rows.T
    for i in range(4):
        spot = jnp.broadcast_to(columns[:, i : i + 1], (LANES, 512)).astype(I32)
        out_ref[i * LANES : (i + 1) * LANES, :] = flag(spot == iota((LANES, 512), 1))


def places(slots_here):
    return pl.pallas_call(place_kernel, out_shape=pltpu.VMEM((512, 512), BF16), name="places")(slots_here)


def join_kernel(heavy_ref, me_ref, got_ref, place_ref, orders_ref, out_ref, report_ref, joined_s):
    lines = [got_ref[pl.ds(t * 320 + 4, 64, stride=5), :] for t in range(4)]
    stretch = [jnp.exp2(line[:, LANES - 1 :].astype(F32)) for line in lines]
    found = (lines[0] + lines[1] + lines[2] + lines[3]).astype(F32)
    lane, member = iota((64, LANES), 1), iota((64, LANES), 0)
    heavy_sums, heavy_counts = [], []
    for h in range(2):
        row = jnp.zeros((64, LANES), F32)
        count = jnp.zeros((64, LANES), F32)
        for line in lines:
            word = line[:, 8 + h : 9 + h]
            scale = jnp.exp2(line[:, 126:127].astype(F32))
            row += jnp.where(lane == 2 * member, decoded(word >> 16, scale), 0.0)
            row += jnp.where(lane == 2 * member + 1, decoded((word << 16) >> 16, scale), 0.0)
            count += jnp.where((member == me_ref[0]) & (lane == 10 + h), line, 0).astype(F32)
        heavy_sums.append(jnp.sum(row, axis=0, keepdims=True))
        heavy_counts.append(jnp.sum(jnp.sum(count, axis=0, keepdims=True), axis=1, keepdims=True))
    above, below = [], []
    for j in range(4):
        words = [got_ref[pl.ds(t * 320 + j, 64, stride=5), :] for t in range(4)]
        above.append(sum(decoded(word >> 16, s) for word, s in zip(words, stretch)))
        below.append(sum(decoded((word << 16) >> 16, s) for word, s in zip(words, stretch)))
    sums = jnp.concatenate(above + below, axis=0)
    high = jnp.floor(found * (1.0 / 128.0)) * 128.0
    low = found - high
    low = jnp.concatenate([jnp.broadcast_to(low[:, j : j + 1], (64, LANES)) for j in range(8)], axis=0).astype(BF16)
    high = jnp.concatenate([jnp.broadcast_to(high[:, j : j + 1], (64, LANES)) for j in range(8)], axis=0)
    high_a, high_b = split2(high)
    sum_a, sum_b = split2(sums)
    right = jnp.concatenate([sum_a, sum_b, low, high_a, high_b], axis=1)

    for i in range(4):
        part = slice(i * LANES, (i + 1) * LANES)
        moved = mm(place_ref[part, :], right)
        total = moved[:, 0:LANES] + moved[:, LANES : 2 * LANES]
        number = moved[:, 2 * LANES : 3 * LANES] + (moved[:, 3 * LANES : 4 * LANES] + moved[:, 4 * LANES :])
        key = iota((LANES, LANES), 0) + i * LANES
        for h in range(2):
            hit = key == heavy_ref[h]
            total = jnp.where(hit, heavy_sums[h], total)
            number = jnp.where(hit, heavy_counts[h], number)
        joined = orders_ref[part, :].astype(F32) * total * lax.rsqrt(1.0 + number)
        joined_s[part, :] = joined
        out_ref[part, :] = joined.astype(BF16)
    report_ref[...] = jnp.concatenate(
        [joined_s[pl.ds(heavy_ref[0], 1), :], joined_s[pl.ds(heavy_ref[1], 1), :]], axis=0
    ).astype(BF16)


def join(heavy_here, member, got, place, orders):
    vmem = pl.BlockSpec(memory_space=pltpu.VMEM)
    smem = pl.BlockSpec(memory_space=pltpu.SMEM)
    return pl.pallas_call(
        join_kernel,
        out_shape=(jax.ShapeDtypeStruct((512, LANES), BF16), jax.ShapeDtypeStruct((2, LANES), BF16)),
        in_specs=[smem, smem, vmem, vmem, vmem],
        scratch_shapes=[pltpu.VMEM((512, LANES), F32)],
        name="join",
    )(heavy_here, member.reshape(1), near(got), near(place), orders)


def swap(x):
    return lax.all_to_all(x, GROUP, split_axis=0, concat_axis=0, tiled=True)


def body(measures, row_keys, orders, heavy_keys, key_slot):
    x, t, low, core, y = (lax.axis_index(name) for name in AXES)
    device = (((x * 4 + t) * 2 + low) * 2 + core) * 4 + y
    owner = ((x * 4 + y) * 2 + low) * 2 + core
    got = swap(pack(row_keys, key_slot, heavy_keys, measures).reshape(64, 1, -1)).reshape(-1, LANES)
    labels = labels_of(owner, key_slot)
    words, *rows = owner_sums(t, got, labels)
    got = lax.all_to_all(words.reshape(256, 1, 640), ("t",) + GROUP, split_axis=0, concat_axis=0, tiled=True)
    got = got.reshape(1280, LANES)
    slot_rows = sum(
        lax.ppermute(rows[i], ("t", "y"), [(4 * a + b, 4 * b + (a + i) % 4) for a in range(4) for b in range(4)])
        for i in range(4)
    )
    heavy_here = lax.dynamic_slice_in_dim(heavy_keys, device * 2, 2) - device * 512
    slots_here = lax.dynamic_slice_in_dim(key_slot, device * 512, 512).reshape(4, LANES)
    result, report = join(heavy_here, ((x * 2 + low) * 2 + core) * 4 + y, got, places(slots_here), orders)
    return result, report, slot_rows.reshape(512)


def solution(mesh):
    split = Mesh(mesh.devices.reshape(4, 4, 2, 2, 4), AXES)
    return jax.shard_map(
        body,
        mesh=split,
        in_specs=(P(AXES, None), P(AXES), P(AXES, None), P(), P()),
        out_specs=(P(AXES, None), P(AXES, None), P(AXES)),
        check_vma=False,
    )
```
